512 devices in a mesh: tm: 64 (over z, y), space: 8 (over x, core).
Axes of the slice: x: 4, y: 8, z: 8, core: 2. Of those that a mesh axis runs over, the one named last changes fastest.
Arguments:
- links: float32 [2, 3, 3, 256, 32768], P(None, None, None, 'tm', 'space'), may hold values from -1 to 1, as said below
Outputs:
- ploop: float32 [2, 32768], P(None, ('space', 'tm'))
- loop_stats: float32 [3], replicated
The draws below stay inside these ranges and needn't reach their ends.
Inputs may be any that keep to these rules, and one draw needn't show every extreme that they name: `links`: every link matrix is special unitary.
All inputs are finite; a program needn't handle non-finite values.
Results may differ from the reference program's by a relative error of at most 0.00014.
Values sent between devices are 32-bit elements; how exact they have to be, the bound alone decides.
A program may use at most 64 MiB of HBM per device.

```python
import jax
import jax.numpy as jnp
from jax import lax

NT = 256
NS = 32768


def inner_prod(first, second):
    real = jnp.sum(first[0] * second[0] + first[1] * second[1], axis=0)
    imag = jnp.sum(first[0] * second[1] - first[1] * second[0], axis=0)
    return (real, imag)


def unit_row(row):
    length = jnp.sqrt(jnp.maximum(jnp.sum(row[0] * row[0] + row[1] * row[1], axis=0), 1e-06))
    return row / length[None, None]


def draw_links(key, part):
    key_noise, key_size = jax.random.split(key)
    noise = jax.random.normal(key_noise, (2, 3, 3, NT, NS), jnp.float32)
    strength = jnp.exp(jax.random.uniform(key_size, (NT, NS), jnp.float32, jnp.log(0.05), jnp.log(0.3)))
    unit = jnp.stack([jnp.eye(3, dtype=jnp.float32), jnp.zeros((3, 3), jnp.float32)])
    matrix = unit[:, :, :, None, None] + noise * strength[None, None, None]
    first = unit_row(matrix[:, 0])
    second = matrix[:, 1]
    real, imag = inner_prod(first, second)
    second = jnp.stack([second[0] - (real * first[0] - imag * first[1]), second[1] - (real * first[1] + imag * first[0])])
    second = unit_row(second)

    def cross_part(j, k):
        real_part = first[0, j] * second[0, k] - first[1, j] * second[1, k] - (first[0, k] * second[0, j] - first[1, k] * second[1, j])
        imag_part = first[0, j] * second[1, k] + first[1, j] * second[0, k] - (first[0, k] * second[1, j] + first[1, k] * second[0, j])
        return (real_part, -imag_part)
    parts = [cross_part(1, 2), cross_part(2, 0), cross_part(0, 1)]
    third = jnp.stack([jnp.stack([p[0] for p in parts]), jnp.stack([p[1] for p in parts])])
    return jnp.stack([first, second, third], axis=1)


def setup_inputs(seed: int = 0) -> dict:
    key_of = jax.random.split(jax.random.key(seed), 2)
    links = draw_links(jax.random.fold_in(key_of[1], 71), 0)
    return {"links": links}


def cmul(left, right):
    def prod(first, second):
        return jnp.sum(first[:, :, None, :] * second[None, :, :, :], axis=1)
    return jnp.stack([prod(left[0], right[0]) - prod(left[1], right[1]),
                      prod(left[0], right[1]) + prod(left[1], right[0])])


def reference(links):
    def step(index, acc):
        return cmul(acc, lax.dynamic_index_in_dim(links, index, 3, keepdims=False))
    whole = lax.fori_loop(1, NT, step, links[:, :, :, 0, :])
    ploop = (whole[:, 0, 0] + whole[:, 1, 1] + whole[:, 2, 2]) / 3.0
    mean_re = jnp.sum(ploop[0]) / NS
    mean_im = jnp.sum(ploop[1]) / NS
    square = jnp.sum(ploop[0] * ploop[0] + ploop[1] * ploop[1]) / NS
    stats = jnp.stack([mean_re, mean_im, square - mean_re * mean_re - mean_im * mean_im])
    return ploop, stats
```

```python
import jax
import jax.numpy as jnp
from jax import lax
from jax.experimental import pallas as pl
from jax.experimental.pallas import tpu as pltpu
from jax.sharding import PartitionSpec as P

MESH = pl.DeviceIdType.MESH
LANES = 128
NY = 8
NZ = 8
NCLASS = 4
NSPACE = 8
ROWS = 2
FAR_FIRST = (4, 3, 5, 2, 6, 1, 7)
PAIRS = (2, 1, 3, 0)


def third_row(a, b):
    row = []
    for i, j in ((1, 2), (2, 0), (0, 1)):
        re = (a[i][0] * b[j][0] - a[i][1] * b[j][1]) - (a[j][0] * b[i][0] - a[j][1] * b[i][1])
        im = (a[j][0] * b[i][1] + a[j][1] * b[i][0]) - (a[i][0] * b[j][1] + a[i][1] * b[j][0])
        row.append((re, im))
    return row


def times(left, right):
    out = []
    for row in left:
        new = []
        for c in range(3):
            re = im = None
            for k in range(3):
                lr, li = row[k]
                rr, ri = right[k][c]
                tr = lr * rr - li * ri
                ti = lr * ri + li * rr
                re = tr if re is None else re + tr
                im = ti if im is None else im + ti
            new.append((re, im))
        out.append(new)
    return out


def full(two):
    return [two[0], two[1], third_row(two[0], two[1])]


def kernel(links, ploop_out, stats_out, lbuf, ysend, yrecv, zsend, zrecv, prow, arecv, brecv,
           load_sem, ysend_sem, yrecv_sem, zsend_sem, zrecv_sem, psend_sem, precv_sem,
           asend_sem, arecv_sem, bsend_sem, brecv_sem):
    tm = lax.axis_index("tm")
    s = lax.axis_index("space")
    z = lax.div(tm, NY)
    y = lax.rem(tm, NY)

    def at(dz, dy, ds):
        return (lax.rem(z + dz + NZ, NZ) * NY + lax.rem(y + dy, NY), lax.rem(s + ds, NSPACE))

    loads = {}
    for k in range(4):
        for t in range(4):
            m = lax.rem(lax.div(y, 2) + PAIRS[k], 4)
            loads[k, t] = pltpu.make_async_copy(
                links.at[:, :, m, t], lbuf.at[k, t], load_sem.at[k, t])
            loads[k, t].start()

    barrier = pltpu.get_barrier_semaphore()

    def greet(where):
        pl.semaphore_signal(barrier, inc=1, device_id=where, device_id_type=MESH)

    for d in FAR_FIRST:
        greet(at(0, d, 0))
    for d in FAR_FIRST:
        greet(at(d, 0, 0))
    for dz in (0, 1, -1, 2):
        for d in range(1, NSPACE):
            greet(at(dz, 0, d))

    def local(k):
        for t in range(4):
            loads[k, t].wait()

        def matrix(t, rows):
            return [[(lbuf[k, t, r * 3 + c], lbuf[k, t, 9 + r * 3 + c]) for c in range(3)]
                    for r in range(rows)]

        acc = matrix(0, ROWS)
        for t in range(1, 4):
            acc = times(acc, matrix(t, 3))
        for h in range(2):
            for r in range(ROWS):
                for c in range(3):
                    for p in range(2):
                        ysend[k, h, (r * 3 + c) * 2 + p] = acc[r][c][p][4 * h:4 * h + 4]

    def ycopy(k, h, owner):
        return pltpu.make_async_remote_copy(
            src_ref=ysend.at[k, h], dst_ref=yrecv.at[y],
            send_sem=ysend_sem.at[k, h], recv_sem=yrecv_sem.at[y],
            device_id=(z * NY + owner, s), device_id_type=MESH)

    for k in range(4):
        local(k)
        if k == 0:
            pl.semaphore_wait(barrier, 2 * 7 + 4 * (NSPACE - 1))
        m = lax.rem(lax.div(y, 2) + PAIRS[k], 4)
        for h in range(2):
            owner = m * 2 + h
            if k < 3:
                ycopy(k, h, owner).start()
            else:
                @pl.when(owner != y)
                def _():
                    ycopy(k, h, owner).start()

                @pl.when(owner == y)
                def _():
                    yrecv[y] = ysend[k, h]

    acc = None
    for j in range(NY):
        @pl.when(y != j)
        def _():
            pltpu.make_async_remote_copy(
                src_ref=ysend.at[0, 0], dst_ref=yrecv.at[j],
                send_sem=ysend_sem.at[0, 0], recv_sem=yrecv_sem.at[j],
                device_id=(tm, s), device_id_type=MESH).wait_recv()

        two = [[(yrecv[j, (r * 3 + c) * 2], yrecv[j, (r * 3 + c) * 2 + 1]) for c in range(3)]
               for r in range(ROWS)]
        acc = two if acc is None else times(acc, full(two))
    for r in range(ROWS):
        for c in range(3):
            for p in range(2):
                zsend[(r * 3 + c) * 2 + p] = acc[r][c][p].reshape(4, 1, LANES)

    cls = lax.rem(z, NCLASS)
    zrecv[:, pl.ds(z, 1)] = zsend[:, pl.ds(cls, 1)]

    def zcopy(d):
        want = lax.rem(z + d, NCLASS)
        return pltpu.make_async_remote_copy(
            src_ref=zsend.at[:, want], dst_ref=zrecv.at[:, z],
            send_sem=zsend_sem.at[d], recv_sem=zrecv_sem,
            device_id=at(d, 0, 0), device_id_type=MESH)

    for d in FAR_FIRST:
        zcopy(d).start()
    rest = zrecv.at[:, pl.ds(0, NZ - 1)]
    pltpu.make_async_copy(rest, rest, zrecv_sem).wait()

    acc = None
    for j in range(NZ):
        two = [[(zrecv[(r * 3 + c) * 2, j], zrecv[(r * 3 + c) * 2 + 1, j]) for c in range(3)]
               for r in range(ROWS)]
        acc = two if acc is None else times(acc, full(two))
    whole = full(acc)
    re = (whole[0][0][0] + whole[1][1][0] + whole[2][2][0]) / 3.0
    im = (whole[0][0][1] + whole[1][1][1] + whole[2][2][1]) / 3.0

    half = lax.rem(y, 2)
    holder = lax.div(z, NCLASS) == half
    pcopy = pltpu.make_async_remote_copy(
        src_ref=prow, dst_ref=prow, send_sem=psend_sem, recv_sem=precv_sem,
        device_id=(tm + 1 - 2 * half, s), device_id_type=MESH)

    @pl.when(holder)
    def _():
        prow[0:1] = re
        prow[1:2] = im
        pcopy.start()

    lane = lax.broadcasted_iota(jnp.int32, (1, LANES), 1)
    sums = jnp.where(lane == 0, jnp.sum(re, axis=1, keepdims=True),
                     jnp.where(lane == 1, jnp.sum(im, axis=1, keepdims=True),
                               jnp.sum(re * re + im * im, axis=1, keepdims=True)))
    arecv[y] = sums

    def acopy(d):
        return pltpu.make_async_remote_copy(
            src_ref=arecv.at[y], dst_ref=arecv.at[y], send_sem=asend_sem.at[d],
            recv_sem=arecv_sem, device_id=at(0, d, 0), device_id_type=MESH)

    for d in FAR_FIRST:
        acopy(d).start()
    rest_a = arecv.at[pl.ds(0, NY - 1)]
    pltpu.make_async_copy(rest_a, rest_a, arecv_sem).wait()
    total = jnp.sum(arecv[...], axis=0)
    mine = cls * NSPACE + s
    brecv[mine] = total

    def bcopy(i, dz, d):
        return pltpu.make_async_remote_copy(
            src_ref=brecv.at[mine], dst_ref=brecv.at[mine], send_sem=bsend_sem.at[i],
            recv_sem=brecv_sem, device_id=at(dz, 0, d), device_id_type=MESH)

    bcopies = [bcopy(i * NSPACE + d, dz, d)
               for i, dz in enumerate((-2, -1, 1, 0)) for d in range(NSPACE) if dz != 0 or d != 0]
    for copy in bcopies:
        copy.start()

    @pl.when(jnp.logical_not(holder))
    def _():
        pcopy.wait_recv()

    both = prow[...]
    ploop_out[...] = jnp.where(half == 0, both[:, :64], both[:, 64:])

    rest_b = brecv.at[pl.ds(0, NCLASS * NSPACE - 1)]
    pltpu.make_async_copy(rest_b, rest_b, brecv_sem).wait()
    grand = jnp.sum(brecv[...], axis=0) / (NY * NCLASS * NSPACE * LANES)
    mean_re = grand[0, 0]
    mean_im = grand[0, 1]
    square = grand[0, 2]
    stats_out[0] = mean_re
    stats_out[1] = mean_im
    stats_out[2] = square - mean_re * mean_re - mean_im * mean_im

    for k in range(4):
        m = lax.rem(lax.div(y, 2) + PAIRS[k], 4)
        for h in range(2):
            if k < 3:
                ycopy(k, h, m * 2 + h).wait_send()
            else:
                @pl.when(m * 2 + h != y)
                def _():
                    ycopy(k, h, m * 2 + h).wait_send()
    for d in FAR_FIRST:
        zcopy(d).wait_send()
        acopy(d).wait_send()
    for copy in bcopies:
        copy.wait_send()

    @pl.when(holder)
    def _():
        pcopy.wait_send()


def on_device(links):
    times_here, sites = links.shape[3:]
    rows = sites // LANES
    view = links.reshape(18, times_here, rows, LANES).transpose(0, 2, 1, 3)
    view = view.reshape(18, 8, 4, times_here, LANES)
    f32 = jnp.float32
    dma = pltpu.SemaphoreType.DMA
    return pl.pallas_call(
        kernel,
        out_shape=(jax.ShapeDtypeStruct((2, sites // 64), f32), jax.ShapeDtypeStruct((3,), f32)),
        in_specs=[pl.BlockSpec(memory_space=pl.ANY)],
        out_specs=(pl.BlockSpec(memory_space=pltpu.VMEM), pl.BlockSpec(memory_space=pltpu.SMEM)),
        scratch_shapes=[
            pltpu.VMEM((4, 4, 18, 8, LANES), f32),
            pltpu.VMEM((4, 2, 12, 4, LANES), f32),
            pltpu.VMEM((NY, 12, 4, LANES), f32),
            pltpu.VMEM((12, 4, 1, LANES), f32),
            pltpu.VMEM((12, NZ, 1, LANES), f32),
            pltpu.VMEM((2, LANES), f32),
            pltpu.VMEM((NY, 1, LANES), f32),
            pltpu.VMEM((NCLASS * NSPACE, 1, LANES), f32),
            dma((4, 4)), dma((4, 2)), dma((NY,)), dma((NZ,)), dma, dma, dma,
            dma((NY,)), dma, dma((NCLASS * NSPACE,)), dma,
        ],
        compiler_params=pltpu.CompilerParams(collective_id=0, has_side_effects=True),
    )(view)


def solution(mesh):
    return jax.shard_map(
        on_device, mesh=mesh, in_specs=(P(None, None, None, "tm", "space"),),
        out_specs=(P(None, ("space", "tm")), P()), check_vma=False)
```

```python
import jax
import jax.numpy as jnp
from jax import lax
from jax.experimental import pallas as pl
from jax.experimental.pallas import tpu as pltpu
from jax.sharding import PartitionSpec as P

MESH = pl.DeviceIdType.MESH
LANES = 128
NY = 8
NZ = 8
NCLASS = 4
NSPACE = 8
ROWS = 2
FAR_FIRST = (4, 3, 5, 2, 6, 1, 7)
PAIRS = (2, 1, 3, 0)


def third_row(a, b):
    row = []
    for i, j in ((1, 2), (2, 0), (0, 1)):
        re = (a[i][0] * b[j][0] - a[i][1] * b[j][1]) - (a[j][0] * b[i][0] - a[j][1] * b[i][1])
        im = (a[j][0] * b[i][1] + a[j][1] * b[i][0]) - (a[i][0] * b[j][1] + a[i][1] * b[j][0])
        row.append((re, im))
    return row


def times(left, right):
    out = []
    for row in left:
        new = []
        for c in range(3):
            re = im = None
            for k in range(3):
                lr, li = row[k]
                rr, ri = right[k][c]
                tr = lr * rr - li * ri
                ti = lr * ri + li * rr
                re = tr if re is None else re + tr
                im = ti if im is None else im + ti
            new.append((re, im))
        out.append(new)
    return out


def full(two):
    return [two[0], two[1], third_row(two[0], two[1])]


def kernel(links, ploop_out, stats_out, lbuf, ysend, yrecv, zsend, zrecv, prow, arecv, brecv,
           near_sem, load_sem, ysend_sem, yrecv_sem, zsend_sem, zrecv_sem, psend_sem, precv_sem,
           asend_sem, arecv_sem, bsend_sem, brecv_sem):
    tm = lax.axis_index("tm")
    s = lax.axis_index("space")
    z = lax.div(tm, NY)
    y = lax.rem(tm, NY)

    def at(dz, dy, ds):
        return (lax.rem(z + dz + NZ, NZ) * NY + lax.rem(y + dy + NY, NY), lax.rem(s + ds + NSPACE, NSPACE))

    other_core = (tm, s + 1 - 2 * lax.rem(s, 2))
    near = [at(1, 0, 0), at(-1, 0, 0), at(0, 0, 2), at(0, 0, -2), other_core]
    farther = [at(2, 0, 0), at(-2, 0, 0), at(0, 0, 4), other_core]

    def tell(sem, whom):
        for where in whom:
            pl.semaphore_signal(sem, inc=1, device_id=where, device_id_type=MESH)

    barrier = pltpu.get_barrier_semaphore()
    greeted = [at(0, d, 0) for d in FAR_FIRST] + near
    tell(barrier, greeted)

    pairs = [lax.rem(lax.div(y, 2) + step, 4) for step in PAIRS]
    for k, m in enumerate(pairs):
        for t in range(4):
            pltpu.make_async_copy(links.at[:, :, m, t], lbuf.at[k, t], load_sem.at[k]).start()

    def local(k):
        pltpu.make_async_copy(lbuf.at[k], lbuf.at[k], load_sem.at[k]).wait()

        def matrix(t, rows):
            return [[(lbuf[k, t, r * 3 + c], lbuf[k, t, 9 + r * 3 + c]) for c in range(3)]
                    for r in range(rows)]

        acc = matrix(0, ROWS)
        for t in range(1, 4):
            acc = times(acc, matrix(t, 3))
        for h in range(2):
            for r in range(ROWS):
                for c in range(3):
                    for p in range(2):
                        ysend[pairs[k] * 2 + h, (r * 3 + c) * 2 + p] = acc[r][c][p][4 * h:4 * h + 4]

    def ycopy(d):
        owner = lax.rem(y + d + NY, NY)
        pltpu.make_async_remote_copy(
            src_ref=ysend.at[owner], dst_ref=yrecv.at[y], send_sem=ysend_sem,
            recv_sem=yrecv_sem.at[y], device_id=(z * NY + owner, s), device_id_type=MESH).start()

    for k in range(4):
        local(k)
    pl.semaphore_wait(barrier, len(greeted))
    tell(near_sem.at[0], near)
    for d in FAR_FIRST:
        ycopy(d)
    yrecv[y] = ysend[y]
    pl.semaphore_wait(near_sem.at[0], len(near))
    tell(near_sem.at[1], farther)

    acc = None
    for j in range(NY):
        @pl.when(y != j)
        def _():
            pltpu.make_async_remote_copy(
                src_ref=ysend.at[0], dst_ref=yrecv.at[j],
                send_sem=ysend_sem, recv_sem=yrecv_sem.at[j],
                device_id=(tm, s), device_id_type=MESH).wait_recv()

        two = [[(yrecv[j, (r * 3 + c) * 2], yrecv[j, (r * 3 + c) * 2 + 1]) for c in range(3)]
               for r in range(ROWS)]
        acc = two if acc is None else times(acc, full(two))
    for r in range(ROWS):
        for c in range(3):
            for p in range(2):
                zsend[(r * 3 + c) * 2 + p] = acc[r][c][p].reshape(4, 1, LANES)

    pl.semaphore_wait(near_sem.at[1], len(farther))
    tell(near_sem.at[2], [other_core])
    cls = lax.rem(z, NCLASS)
    zrecv[:, pl.ds(z, 1)] = zsend[:, pl.ds(cls, 1)]

    def zcopy(d):
        want = lax.rem(z + d, NCLASS)
        return pltpu.make_async_remote_copy(
            src_ref=zsend.at[:, want], dst_ref=zrecv.at[:, z],
            send_sem=zsend_sem, recv_sem=zrecv_sem,
            device_id=at(d, 0, 0), device_id_type=MESH)

    for d in FAR_FIRST:
        zcopy(d).start()
    rest = zrecv.at[:, pl.ds(0, NZ - 1)]
    pltpu.make_async_copy(rest, rest, zrecv_sem).wait()
    acc = None
    for j in range(NZ):
        two = [[(zrecv[(r * 3 + c) * 2, j], zrecv[(r * 3 + c) * 2 + 1, j]) for c in range(3)]
               for r in range(ROWS)]
        acc = two if acc is None else times(acc, full(two))
    whole = full(acc)
    re = (whole[0][0][0] + whole[1][1][0] + whole[2][2][0]) / 3.0
    im = (whole[0][0][1] + whole[1][1][1] + whole[2][2][1]) / 3.0

    half = lax.rem(y, 2)
    holder = lax.div(z, NCLASS) == half
    pcopy = pltpu.make_async_remote_copy(
        src_ref=prow, dst_ref=prow, send_sem=psend_sem, recv_sem=precv_sem,
        device_id=(tm + 1 - 2 * half, s), device_id_type=MESH)

    @pl.when(holder)
    def _():
        prow[0:1] = re
        prow[1:2] = im
        pcopy.start()

    lane = lax.broadcasted_iota(jnp.int32, (1, LANES), 1)
    sums = jnp.where(lane == 0, jnp.sum(re, axis=1, keepdims=True),
                     jnp.where(lane == 1, jnp.sum(im, axis=1, keepdims=True),
                               jnp.sum(re * re + im * im, axis=1, keepdims=True)))
    arecv[y] = sums

    def acopy(d):
        return pltpu.make_async_remote_copy(
            src_ref=arecv.at[y], dst_ref=arecv.at[y], send_sem=asend_sem,
            recv_sem=arecv_sem, device_id=at(0, d, 0), device_id_type=MESH)

    for d in FAR_FIRST:
        acopy(d).start()
    rest_a = arecv.at[pl.ds(0, NY - 1)]
    pltpu.make_async_copy(rest_a, rest_a, arecv_sem).wait()
    total = jnp.sum(arecv[...], axis=0)
    mine = cls * NSPACE + s
    brecv[mine] = total

    def bcopy(dz, d):
        return pltpu.make_async_remote_copy(
            src_ref=brecv.at[mine], dst_ref=brecv.at[mine], send_sem=bsend_sem,
            recv_sem=brecv_sem, device_id=at(dz, 0, d), device_id_type=MESH)

    pl.semaphore_wait(near_sem.at[2], 1)
    for dz in (2, -1, 1, 0):
        for d in range(NSPACE):
            if dz != 0 or d != 0:
                bcopy(dz, d).start()

    @pl.when(jnp.logical_not(holder))
    def _():
        pcopy.wait_recv()

    ploop_out[...] = jnp.where(half == 0, prow[:, :64], prow[:, 64:])

    rest_b = brecv.at[pl.ds(0, NCLASS * NSPACE - 1)]
    pltpu.make_async_copy(rest_b, rest_b, brecv_sem).wait()
    grand = jnp.sum(brecv[...], axis=0) / (NY * NCLASS * NSPACE * LANES)
    means = jnp.where(lane < 2, grand * grand, 0.0)
    stats = grand - jnp.where(lane == 2, jnp.sum(means, axis=1, keepdims=True), 0.0)
    stats_out[...] = stats[0, :3]

    for ref, sem in ((ysend.at[pl.ds(0, NY - 1)], ysend_sem), (rest, zsend_sem), (rest_a, asend_sem), (rest_b, bsend_sem)):
        pltpu.make_async_remote_copy(
            src_ref=ref, dst_ref=ref, send_sem=sem, recv_sem=sem,
            device_id=other_core, device_id_type=MESH).wait_send()

    @pl.when(holder)
    def _():
        pcopy.wait_send()


def finish(ploop_in, stats_in, ploop_out, stats_out, sems):
    copies = [pltpu.make_async_copy(ploop_in, ploop_out, sems.at[0]),
              pltpu.make_async_copy(stats_in, stats_out, sems.at[1])]
    for copy in copies:
        copy.start()
    for copy in copies:
        copy.wait()


def on_device(links):
    times_here, sites = links.shape[3:]
    rows = sites // LANES
    view = links.reshape(18, times_here, rows, LANES).transpose(0, 2, 1, 3)
    view = view.reshape(18, 8, 4, times_here, LANES)
    f32 = jnp.float32
    dma = pltpu.SemaphoreType.DMA
    vmem = pl.BlockSpec(memory_space=pltpu.VMEM)
    ploop, stats = pl.pallas_call(
        kernel,
        out_shape=(pltpu.VMEM((2, sites // 64), f32), pltpu.VMEM((3,), f32)),
        in_specs=[pl.BlockSpec(memory_space=pl.ANY)],
        out_specs=(vmem, vmem),
        scratch_shapes=[
            pltpu.VMEM((4, 4, 18, 8, LANES), f32),
            pltpu.VMEM((NY, 12, 4, LANES), f32),
            pltpu.VMEM((NY, 12, 4, LANES), f32),
            pltpu.VMEM((12, 4, 1, LANES), f32),
            pltpu.VMEM((12, NZ, 1, LANES), f32),
            pltpu.VMEM((2, LANES), f32),
            pltpu.VMEM((NY, 1, LANES), f32),
            pltpu.VMEM((NCLASS * NSPACE, 1, LANES), f32),
            pltpu.SemaphoreType.REGULAR((3,)),
            dma((4,)), dma, dma((NY,)), dma, dma, dma, dma, dma, dma, dma, dma,
        ],
        compiler_params=pltpu.CompilerParams(collective_id=0, has_side_effects=True),
    )(view)
    hbm = pl.BlockSpec(memory_space=pl.ANY)
    return pl.pallas_call(
        finish,
        out_shape=(jax.ShapeDtypeStruct((2, sites // 64), f32), jax.ShapeDtypeStruct((3,), f32)),
        in_specs=[vmem, vmem],
        out_specs=(hbm, hbm),
        scratch_shapes=[dma((2,))],
    )(*(pltpu.with_memory_space_constraint(x, pltpu.VMEM) for x in (ploop, stats)))


def solution(mesh):
    return jax.shard_map(
        on_device, mesh=mesh, in_specs=(P(None, None, None, "tm", "space"),),
        out_specs=(P(None, ("space", "tm")), P()), check_vma=False)
```

```python
import jax
import jax.numpy as jnp
from jax import lax
from jax.experimental import pallas as pl
from jax.experimental.pallas import tpu as pltpu
from jax.sharding import PartitionSpec as P

MESH = pl.DeviceIdType.MESH
LANES = 128
NY = 8
NZ = 8
NCLASS = 4
NX = 4
NSPACE = 8
ROWS = 2
FAR_FIRST = (4, 3, 5, 2, 6, 1, 7)
PAIRS = (2, 1, 3, 0)


def third_row(a, b):
    row = []
    for i, j in ((1, 2), (2, 0), (0, 1)):
        re = (a[i][0] * b[j][0] - a[i][1] * b[j][1]) - (a[j][0] * b[i][0] - a[j][1] * b[i][1])
        im = (a[j][0] * b[i][1] + a[j][1] * b[i][0]) - (a[i][0] * b[j][1] + a[i][1] * b[j][0])
        row.append((re, im))
    return row


def times(left, right):
    out = []
    for row in left:
        new = []
        for c in range(3):
            re = im = None
            for k in range(3):
                lr, li = row[k]
                rr, ri = right[k][c]
                tr = lr * rr - li * ri
                ti = lr * ri + li * rr
                re = tr if re is None else re + tr
                im = ti if im is None else im + ti
            new.append((re, im))
        out.append(new)
    return out


def full(two):
    return [two[0], two[1], third_row(two[0], two[1])]


def kernel(links, ploop_out, stats_out, lbuf, ysend, yrecv, zsend, zrecv, phold, prow, arecv, brecv,
           near_sem, load_sem, ysend_sem, yrecv_sem, zsend_sem, zrecv_sem, psend_sem, precv_sem,
           asend_sem, arecv_sem, bsend_sem, brecv_sem):
    tm = lax.axis_index("tm")
    s = lax.axis_index("space")
    z = lax.div(tm, NY)
    y = lax.rem(tm, NY)
    x = lax.div(s, 2)
    core = lax.rem(s, 2)

    def at(dz, dy, dx, to):
        return (lax.rem(z + dz + NZ, NZ) * NY + lax.rem(y + dy + NY, NY), lax.rem(x + dx, NX) * 2 + to)

    def tell(sem, whom):
        for where in whom:
            pl.semaphore_signal(sem, inc=1, device_id=where, device_id_type=MESH)

    ring = [at(0, d, 0, 1) for d in FAR_FIRST]
    near = [at(1, 0, 0, 1), at(-1, 0, 0, 1), at(0, 0, 1, 1), at(0, 0, 3, 1)]
    farther = [at(2, 0, 0, 1), at(-2, 0, 0, 1), at(0, 0, 2, 1)]
    barrier = pltpu.get_barrier_semaphore()

    @pl.when(core == 1)
    def _():
        tell(barrier, ring + [at(0, d, 0, 0) for d in FAR_FIRST] + near + [at(0, 0, 0, 0)])

    @pl.when(core == 0)
    def _():
        tell(barrier, [at(0, 0, 0, 1)])

    pairs = [lax.rem(lax.div(y, 2) + step, 4) for step in PAIRS]
    for k, m in enumerate(pairs):
        for t in range(4):
            pltpu.make_async_copy(links.at[:, :, m, t], lbuf.at[k, t], load_sem.at[k]).start()

    def local(k):
        pltpu.make_async_copy(lbuf.at[k], lbuf.at[k], load_sem.at[k]).wait()

        def matrix(t, rows):
            return [[(lbuf[k, t, r * 3 + c], lbuf[k, t, 9 + r * 3 + c]) for c in range(3)]
                    for r in range(rows)]

        acc = matrix(0, ROWS)
        for t in range(1, 4):
            acc = times(acc, matrix(t, 3))
        for h in range(2):
            for r in range(ROWS):
                for c in range(3):
                    for p in range(2):
                        ysend[pairs[k] * 2 + h, (r * 3 + c) * 2 + p] = acc[r][c][p][4 * h:4 * h + 4]

    def ycopy(d):
        owner = lax.rem(y + d, NY)
        pltpu.make_async_remote_copy(
            src_ref=ysend.at[owner], dst_ref=yrecv.at[y, :, pl.ds(pl.multiple_of(core * NCLASS, NCLASS), NCLASS)],
            send_sem=ysend_sem, recv_sem=yrecv_sem.at[y, core], device_id=at(0, d, 0, 1), device_id_type=MESH).start()

    for k in range(4):
        local(k)

    def sent(ref, sem):
        pltpu.make_async_remote_copy(
            src_ref=ref, dst_ref=ref, send_sem=sem, recv_sem=sem,
            device_id=at(0, 0, 0, 1 - core), device_id_type=MESH).wait_send()

    def arrived(ref, sem):
        pltpu.make_async_copy(ref, ref, sem).wait()

    half = lax.rem(y, 2)
    holder = lax.div(z, NCLASS) == half
    lane = lax.broadcasted_iota(jnp.int32, (1, LANES), 1)

    @pl.when(core == 0)
    def _():
        pl.semaphore_wait(barrier, NY)
        for d in FAR_FIRST + (0,):
            ycopy(d)
        arrived(prow, precv_sem)
        arrived(brecv, brecv_sem)
        sent(ysend, ysend_sem)

    @pl.when(core == 1)
    def _():
        pl.semaphore_wait(barrier, len(ring) + len(near) + 1)
        tell(near_sem.at[0], near)
        for d in FAR_FIRST:
            ycopy(d)
        yrecv[y, :, NCLASS:] = ysend[y]
        pl.semaphore_wait(near_sem.at[0], len(near))
        tell(near_sem.at[1], farther)

        acc = None
        for j in range(NY):
            arrived(yrecv.at[j, :, pl.ds(0, NCLASS)], yrecv_sem.at[j, 0])

            @pl.when(y != j)
            def _():
                arrived(yrecv.at[j, :, pl.ds(NCLASS, NCLASS)], yrecv_sem.at[j, 1])

            two = [[(yrecv[j, (r * 3 + c) * 2], yrecv[j, (r * 3 + c) * 2 + 1]) for c in range(3)]
                   for r in range(ROWS)]
            acc = two if acc is None else times(acc, full(two))
        for r in range(ROWS):
            for c in range(3):
                for p in range(2):
                    for i in range(NCLASS):
                        for to in range(2):
                            row = NCLASS * to + i
                            zsend[(r * 3 + c) * 2 + p, i, to:to + 1] = acc[r][c][p][row:row + 1]

        pl.semaphore_wait(near_sem.at[1], len(farther))
        tell(near_sem.at[2], [at(0, 0, 2, 1)])
        cls = lax.rem(z, NCLASS)
        for d in FAR_FIRST:
            pltpu.make_async_remote_copy(
                src_ref=zsend.at[:, lax.rem(z + d, NCLASS)], dst_ref=zrecv.at[:, z],
                send_sem=zsend_sem, recv_sem=zrecv_sem, device_id=at(d, 0, 0, 1), device_id_type=MESH).start()
        zrecv[:, z] = zsend[:, cls]
        arrived(zrecv.at[:, pl.ds(0, NZ - 1)], zrecv_sem)

        acc = None
        for j in range(NZ):
            two = [[(zrecv[(r * 3 + c) * 2, j], zrecv[(r * 3 + c) * 2 + 1, j]) for c in range(3)]
                   for r in range(ROWS)]
            acc = two if acc is None else times(acc, full(two))
        whole = full(acc)
        re = (whole[0][0][0] + whole[1][1][0] + whole[2][2][0]) / 3.0
        im = (whole[0][0][1] + whole[1][1][1] + whole[2][2][1]) / 3.0

        def total(value):
            return jnp.sum(jnp.sum(value, axis=1, keepdims=True), axis=0, keepdims=True)

        sums = jnp.where(lane == 0, total(re), jnp.where(lane == 1, total(im), total(re * re + im * im)))
        arecv[y] = sums
        for d in FAR_FIRST:
            pltpu.make_async_remote_copy(
                src_ref=arecv.at[y], dst_ref=arecv.at[y], send_sem=asend_sem,
                recv_sem=arecv_sem, device_id=at(0, d, 0, 1), device_id_type=MESH).start()

        @pl.when(holder)
        def _():
            for to in range(2):
                phold[to, 0:1] = re[to:to + 1]
                phold[to, 1:2] = im[to:to + 1]
            other = 1 - 2 * half
            for to, where in ((0, (tm, s - 1)), (0, (tm + other, s - 1)), (1, (tm + other, s))):
                pltpu.make_async_remote_copy(
                    src_ref=phold.at[to], dst_ref=prow, send_sem=psend_sem, recv_sem=precv_sem,
                    device_id=where, device_id_type=MESH).start()
            prow[...] = phold[1]

        arrived(arecv.at[pl.ds(0, NY - 1)], arecv_sem)
        mine = cls * NX + x
        brecv[mine] = jnp.sum(arecv[...], axis=0)
        pl.semaphore_wait(near_sem.at[2], 1)
        for dz in (2, -1, 1, 0):
            for dx in (2, 1, 3, 0):
                for to in (0, 1):
                    if dz != 0 or dx != 0 or to == 0:
                        pltpu.make_async_remote_copy(
                            src_ref=brecv.at[mine], dst_ref=brecv.at[mine], send_sem=bsend_sem,
                            recv_sem=brecv_sem, device_id=at(dz, 0, dx, to), device_id_type=MESH).start()

        @pl.when(jnp.logical_not(holder))
        def _():
            arrived(prow, precv_sem)

        arrived(brecv.at[pl.ds(0, NCLASS * NX - 1)], brecv_sem)
        sent(ysend.at[pl.ds(0, NY - 1)], ysend_sem)
        sent(zrecv.at[:, pl.ds(0, NZ - 1)], zsend_sem)
        sent(arecv.at[pl.ds(0, NY - 1)], asend_sem)
        sent(brecv, bsend_sem)
        sent(brecv.at[pl.ds(0, NCLASS * NX - 1)], bsend_sem)

        @pl.when(holder)
        def _():
            for _ in range(3):
                sent(prow, psend_sem)

    ploop_out[...] = jnp.where(half == 0, prow[:, :64], prow[:, 64:])
    grand = jnp.sum(brecv[...], axis=0) / (NY * NCLASS * NSPACE * LANES)
    means = jnp.where(lane < 2, grand * grand, 0.0)
    stats = grand - jnp.where(lane == 2, jnp.sum(means, axis=1, keepdims=True), 0.0)
    stats_out[...] = stats[0, :3]


def finish(ploop_in, stats_in, ploop_out, stats_out, sems):
    copies = [pltpu.make_async_copy(ploop_in, ploop_out, sems.at[0]),
              pltpu.make_async_copy(stats_in, stats_out, sems.at[1])]
    for copy in copies:
        copy.start()
    for copy in copies:
        copy.wait()


def on_device(links):
    times_here, sites = links.shape[3:]
    rows = sites // LANES
    view = links.reshape(18, times_here, rows, LANES).transpose(0, 2, 1, 3)
    view = view.reshape(18, 8, 4, times_here, LANES)
    f32 = jnp.float32
    dma = pltpu.SemaphoreType.DMA
    vmem = pl.BlockSpec(memory_space=pltpu.VMEM)
    ploop, stats = pl.pallas_call(
        kernel,
        out_shape=(pltpu.VMEM((2, sites // 64), f32), pltpu.VMEM((3,), f32)),
        in_specs=[pl.BlockSpec(memory_space=pl.ANY)],
        out_specs=(vmem, vmem),
        scratch_shapes=[
            pltpu.VMEM((4, 4, 18, 8, LANES), f32),
            pltpu.VMEM((NY, 12, NCLASS, LANES), f32),
            pltpu.VMEM((NY, 12, 2 * NCLASS, LANES), f32),
            pltpu.VMEM((12, NCLASS, 2, LANES), f32),
            pltpu.VMEM((12, NZ, 2, LANES), f32),
            pltpu.VMEM((2, 2, LANES), f32),
            pltpu.VMEM((2, LANES), f32),
            pltpu.VMEM((NY, 1, LANES), f32),
            pltpu.VMEM((NCLASS * NX, 1, LANES), f32),
            pltpu.SemaphoreType.REGULAR((3,)),
            dma((4,)), dma, dma((NY, 2)), dma, dma, dma, dma, dma, dma, dma, dma,
        ],
        compiler_params=pltpu.CompilerParams(collective_id=0, has_side_effects=True),
    )(view)
    hbm = pl.BlockSpec(memory_space=pl.ANY)
    return pl.pallas_call(
        finish,
        out_shape=(jax.ShapeDtypeStruct((2, sites // 64), f32), jax.ShapeDtypeStruct((3,), f32)),
        in_specs=[vmem, vmem],
        out_specs=(hbm, hbm),
        scratch_shapes=[dma((2,))],
    )(*(pltpu.with_memory_space_constraint(x, pltpu.VMEM) for x in (ploop, stats)))


def solution(mesh):
    return jax.shard_map(
        on_device, mesh=mesh, in_specs=(P(None, None, None, "tm", "space"),),
        out_specs=(P(None, ("space", "tm")), P()), check_vma=False)
```

```python
import jax
import jax.numpy as jnp
from jax import lax
from jax.experimental import pallas as pl
from jax.experimental.pallas import tpu as pltpu
from jax.sharding import PartitionSpec as P

MESH = pl.DeviceIdType.MESH
LANES = 128
NY = 8
NZ = 8
NCLASS = 4
NX = 4
NSPACE = 8
ROWS = 2
COORDS = 8
FAR_FIRST = (4, 3, 5, 2, 6, 1, 7)
PAIRS = (2, 1, 3, 0)


def third_row(a, b):
    row = []
    for i, j in ((1, 2), (2, 0), (0, 1)):
        re = (a[i][0] * b[j][0] - a[i][1] * b[j][1]) - (a[j][0] * b[i][0] - a[j][1] * b[i][1])
        im = (a[j][0] * b[i][1] + a[j][1] * b[i][0]) - (a[i][0] * b[j][1] + a[i][1] * b[j][0])
        row.append((re, im))
    return row


def product(a, b):
    return (a[0] * b[0] - a[1] * b[1], a[0] * b[1] + a[1] * b[0])


def conj_product(a, b):
    return (a[0] * b[0] + a[1] * b[1], a[0] * b[1] - a[1] * b[0])


def project(p):
    q = p[1] * p[1]
    for v in p[2:]:
        q = q + v * v
    below = p[0] < 0.0
    scale = jnp.where(below, 1.0 - p[0], 1.0) / jnp.where(below, jnp.maximum(q, 1e-20), 1.0 + p[0])
    return [jnp.where(below & (q < 1e-20), 1e-10, p[1]) * scale] + [v * scale for v in p[2:]]


def weight(x):
    n = x[0] * x[0]
    for v in x[1:]:
        n = n + v * v
    return 2.0 / (1.0 + n)


def lift(x):
    w = weight(x)
    return [w - 1.0] + [w * v for v in x]


def reflector(x):
    r = weight(x) / (1.0 + x[0] * x[0])
    return (r, r * x[0]), [(1.0, x[0]), (x[1], x[2]), (x[3], x[4])]


def coordinates(two):
    a, b = two
    x = project([v for pair in a for v in pair])
    h, u = reflector(x)
    parts = [conj_product(u[k], b[k]) for k in range(3)]
    k = conj_product(h, (parts[0][0] + parts[1][0] + parts[2][0], parts[0][1] + parts[1][1] + parts[2][1]))
    rest = []
    for j in (1, 2):
        off = product(u[j], k)
        rest += [b[j][0] - off[0], b[j][1] - off[1]]
    return x + project(rest)


def first_rows(v):
    x = v[:5]
    p = lift(x)
    q = lift(v[5:])
    h, u = reflector(x)
    one = conj_product(u[1], (q[0], q[1]))
    two = conj_product(u[2], (q[2], q[3]))
    g = product(h, (one[0] + two[0], one[1] + two[1]))
    off = [product(g, u[k]) for k in range(3)]
    return [[(p[0], p[1]), (p[2], p[3]), (p[4], p[5])],
            [(-off[0][0], -off[0][1]), (q[0] - off[1][0], q[1] - off[1][1]), (q[2] - off[2][0], q[3] - off[2][1])]]


def times(left, right):
    out = []
    for row in left:
        new = []
        for c in range(3):
            re = im = None
            for k in range(3):
                lr, li = row[k]
                rr, ri = right[k][c]
                tr = lr * rr - li * ri
                ti = lr * ri + li * rr
                re = tr if re is None else re + tr
                im = ti if im is None else im + ti
            new.append((re, im))
        out.append(new)
    return out


def full(two):
    return [two[0], two[1], third_row(two[0], two[1])]


def kernel(links, ploop_out, stats_out, lbuf, ysend, yrecv, ymat, zsend, zrecv, zmat, phold, prow, arecv, brecv,
           near_sem, load_sem, ysend_sem, yrecv_sem, zsend_sem, zrecv_sem, psend_sem, precv_sem,
           asend_sem, arecv_sem, bsend_sem, brecv_sem):
    tm = lax.axis_index("tm")
    s = lax.axis_index("space")
    z = lax.div(tm, NY)
    y = lax.rem(tm, NY)
    x = lax.div(s, 2)
    core = lax.rem(s, 2)

    def at(dz, dy, dx, to):
        return (lax.rem(z + dz + NZ, NZ) * NY + lax.rem(y + dy + NY, NY), lax.rem(x + dx, NX) * 2 + to)

    def tell(sem, whom):
        for where in whom:
            pl.semaphore_signal(sem, inc=1, device_id=where, device_id_type=MESH)

    ring = [at(0, d, 0, 1) for d in FAR_FIRST]
    near = [at(1, 0, 0, 1), at(-1, 0, 0, 1), at(0, 0, 1, 1), at(0, 0, 3, 1)]
    farther = [at(2, 0, 0, 1), at(-2, 0, 0, 1), at(0, 0, 2, 1)]
    barrier = pltpu.get_barrier_semaphore()

    @pl.when(core == 1)
    def _():
        tell(barrier, ring + [at(0, d, 0, 0) for d in FAR_FIRST] + near + [at(0, 0, 0, 0)])

    @pl.when(core == 0)
    def _():
        tell(barrier, [at(0, 0, 0, 1)])

    pairs = [lax.rem(lax.div(y, 2) + step, 4) for step in PAIRS]
    for k, m in enumerate(pairs):
        for t in range(4):
            pltpu.make_async_copy(links.at[:, :, m, t], lbuf.at[k, t], load_sem.at[k]).start()

    def local(k):
        pltpu.make_async_copy(lbuf.at[k], lbuf.at[k], load_sem.at[k]).wait()

        def matrix(t, rows):
            return [[(lbuf[k, t, r * 3 + c], lbuf[k, t, 9 + r * 3 + c]) for c in range(3)]
                    for r in range(rows)]

        acc = matrix(0, ROWS)
        for t in range(1, 4):
            acc = times(acc, matrix(t, 3))
        for i, v in enumerate(coordinates(acc)):
            for h in range(2):
                ysend[pairs[k] * 2 + h, i] = v[4 * h:4 * h + 4]

    def ycopy(d):
        owner = lax.rem(y + d, NY)
        pltpu.make_async_remote_copy(
            src_ref=ysend.at[owner], dst_ref=yrecv.at[y, :, pl.ds(pl.multiple_of(core * NCLASS, NCLASS), NCLASS)],
            send_sem=ysend_sem, recv_sem=yrecv_sem.at[y, core], device_id=at(0, d, 0, 1), device_id_type=MESH).start()

    for k in range(4):
        local(k)

    def store(ref, j, mat):
        for r in range(3):
            for c in range(3):
                for p in range(2):
                    ref[j, (r * 3 + c) * 2 + p] = mat[r][c][p]

    def load(ref, j):
        return [[(ref[j, (r * 3 + c) * 2], ref[j, (r * 3 + c) * 2 + 1]) for c in range(3)] for r in range(3)]

    def sent(ref, sem):
        pltpu.make_async_remote_copy(
            src_ref=ref, dst_ref=ref, send_sem=sem, recv_sem=sem,
            device_id=at(0, 0, 0, 1 - core), device_id_type=MESH).wait_send()

    def arrived(ref, sem):
        pltpu.make_async_copy(ref, ref, sem).wait()

    half = lax.rem(y, 2)
    holder = lax.div(z, NCLASS) == half
    lane = lax.broadcasted_iota(jnp.int32, (1, LANES), 1)

    @pl.when(core == 0)
    def _():
        pl.semaphore_wait(barrier, NY)
        for d in FAR_FIRST + (0,):
            ycopy(d)
        arrived(prow, precv_sem)
        arrived(brecv, brecv_sem)
        sent(ysend, ysend_sem)

    @pl.when(core == 1)
    def _():
        pl.semaphore_wait(barrier, len(ring) + len(near) + 1)
        tell(near_sem.at[0], near)
        for d in FAR_FIRST:
            ycopy(d)
        yrecv[y, :, NCLASS:] = ysend[y]
        pl.semaphore_wait(near_sem.at[0], len(near))
        tell(near_sem.at[1], farther)

        for d in FAR_FIRST + (0,):
            j = lax.rem(y + d, NY)
            arrived(yrecv.at[j, :, pl.ds(0, NCLASS)], yrecv_sem.at[j, 0])
            if d != 0:
                arrived(yrecv.at[j, :, pl.ds(NCLASS, NCLASS)], yrecv_sem.at[j, 1])
            store(ymat, j, full(first_rows([yrecv[j, i] for i in range(COORDS)])))
        acc = load(ymat, 0)[:ROWS]
        for j in range(1, NY):
            acc = times(acc, load(ymat, j))
        for i, v in enumerate(coordinates(acc)):
            for k in range(NCLASS):
                for to in range(2):
                    row = NCLASS * to + k
                    zsend[i, k, to:to + 1] = v[row:row + 1]

        pl.semaphore_wait(near_sem.at[1], len(farther))
        tell(near_sem.at[2], [at(0, 0, 2, 1)])
        cls = lax.rem(z, NCLASS)
        for d in FAR_FIRST:
            pltpu.make_async_remote_copy(
                src_ref=zsend.at[:, lax.rem(z + d, NCLASS)], dst_ref=zrecv.at[:, pl.ds(z * 2, 2)],
                send_sem=zsend_sem, recv_sem=zrecv_sem, device_id=at(d, 0, 0, 1), device_id_type=MESH).start()
        zrecv[:, pl.ds(z * 2, 2)] = zsend[:, cls]
        arrived(zrecv.at[:, pl.ds(0, 2 * NZ - 2)], zrecv_sem)

        for j in range(2):
            mat = full(first_rows([zrecv[i, 8 * j:8 * j + 8] for i in range(COORDS)]))
            for r in range(3):
                for c in range(3):
                    for p in range(2):
                        zmat[(r * 3 + c) * 2 + p, 8 * j:8 * j + 8] = mat[r][c][p]

        def slab(j):
            return [[tuple(zmat[(r * 3 + c) * 2 + p, 2 * j:2 * j + 2] for p in range(2)) for c in range(3)]
                    for r in range(3)]

        acc = slab(0)[:ROWS]
        for j in range(1, NZ):
            acc = times(acc, slab(j))
        whole = full(acc)
        re = (whole[0][0][0] + whole[1][1][0] + whole[2][2][0]) / 3.0
        im = (whole[0][0][1] + whole[1][1][1] + whole[2][2][1]) / 3.0

        def total(value):
            return jnp.sum(jnp.sum(value, axis=1, keepdims=True), axis=0, keepdims=True)

        sums = jnp.where(lane == 0, total(re), jnp.where(lane == 1, total(im), total(re * re + im * im)))
        arecv[y] = sums
        for d in FAR_FIRST:
            pltpu.make_async_remote_copy(
                src_ref=arecv.at[y], dst_ref=arecv.at[y], send_sem=asend_sem,
                recv_sem=arecv_sem, device_id=at(0, d, 0, 1), device_id_type=MESH).start()

        @pl.when(holder)
        def _():
            for to in range(2):
                phold[to, 0:1] = re[to:to + 1]
                phold[to, 1:2] = im[to:to + 1]
            other = 1 - 2 * half
            for to, where in ((0, (tm, s - 1)), (0, (tm + other, s - 1)), (1, (tm + other, s))):
                pltpu.make_async_remote_copy(
                    src_ref=phold.at[to], dst_ref=prow, send_sem=psend_sem, recv_sem=precv_sem,
                    device_id=where, device_id_type=MESH).start()
            prow[...] = phold[1]

        arrived(arecv.at[pl.ds(0, NY - 1)], arecv_sem)
        mine = cls * NX + x
        brecv[mine] = jnp.sum(arecv[...], axis=0)
        pl.semaphore_wait(near_sem.at[2], 1)
        for dz in (2, -1, 1, 0):
            for dx in (2, 1, 3, 0):
                for to in (0, 1):
                    if dz != 0 or dx != 0 or to == 0:
                        pltpu.make_async_remote_copy(
                            src_ref=brecv.at[mine], dst_ref=brecv.at[mine], send_sem=bsend_sem,
                            recv_sem=brecv_sem, device_id=at(dz, 0, dx, to), device_id_type=MESH).start()

        @pl.when(jnp.logical_not(holder))
        def _():
            arrived(prow, precv_sem)

        arrived(brecv.at[pl.ds(0, NCLASS * NX - 1)], brecv_sem)
        sent(ysend.at[pl.ds(0, NY - 1)], ysend_sem)
        sent(zrecv.at[:, pl.ds(0, 2 * NZ - 2)], zsend_sem)
        sent(arecv.at[pl.ds(0, NY - 1)], asend_sem)
        sent(brecv, bsend_sem)
        sent(brecv.at[pl.ds(0, NCLASS * NX - 1)], bsend_sem)

        @pl.when(holder)
        def _():
            for _ in range(3):
                sent(prow, psend_sem)

    ploop_out[...] = jnp.where(half == 0, prow[:, :64], prow[:, 64:])
    grand = jnp.sum(brecv[...], axis=0) / (NY * NCLASS * NSPACE * LANES)
    means = jnp.where(lane < 2, grand * grand, 0.0)
    stats = grand - jnp.where(lane == 2, jnp.sum(means, axis=1, keepdims=True), 0.0)
    stats_out[...] = stats[0, :3]


def finish(ploop_in, stats_in, ploop_out, stats_out, sems):
    copies = [pltpu.make_async_copy(ploop_in, ploop_out, sems.at[0]),
              pltpu.make_async_copy(stats_in, stats_out, sems.at[1])]
    for copy in copies:
        copy.start()
    for copy in copies:
        copy.wait()


def on_device(links):
    times_here, sites = links.shape[3:]
    rows = sites // LANES
    view = links.reshape(18, times_here, rows, LANES).transpose(0, 2, 1, 3)
    view = view.reshape(18, 8, 4, times_here, LANES)
    f32 = jnp.float32
    dma = pltpu.SemaphoreType.DMA
    vmem = pl.BlockSpec(memory_space=pltpu.VMEM)
    ploop, stats = pl.pallas_call(
        kernel,
        out_shape=(pltpu.VMEM((2, sites // 64), f32), pltpu.VMEM((3,), f32)),
        in_specs=[pl.BlockSpec(memory_space=pl.ANY)],
        out_specs=(vmem, vmem),
        scratch_shapes=[
            pltpu.VMEM((4, 4, 18, 8, LANES), f32),
            pltpu.VMEM((NY, COORDS, NCLASS, LANES), f32),
            pltpu.VMEM((NY, COORDS, 2 * NCLASS, LANES), f32),
            pltpu.VMEM((NY, 18, 2 * NCLASS, LANES), f32),
            pltpu.VMEM((COORDS, NCLASS, 2, LANES), f32),
            pltpu.VMEM((COORDS, 2 * NZ, LANES), f32),
            pltpu.VMEM((18, 2 * NZ, LANES), f32),
            pltpu.VMEM((2, 2, LANES), f32),
            pltpu.VMEM((2, LANES), f32),
            pltpu.VMEM((NY, 1, LANES), f32),
            pltpu.VMEM((NCLASS * NX, 1, LANES), f32),
            pltpu.SemaphoreType.REGULAR((3,)),
            dma((4,)), dma, dma((NY, 2)), dma, dma, dma, dma, dma, dma, dma, dma,
        ],
        compiler_params=pltpu.CompilerParams(collective_id=0, has_side_effects=True),
    )(view)
    hbm = pl.BlockSpec(memory_space=pl.ANY)
    return pl.pallas_call(
        finish,
        out_shape=(jax.ShapeDtypeStruct((2, sites // 64), f32), jax.ShapeDtypeStruct((3,), f32)),
        in_specs=[vmem, vmem],
        out_specs=(hbm, hbm),
        scratch_shapes=[dma((2,))],
    )(*(pltpu.with_memory_space_constraint(x, pltpu.VMEM) for x in (ploop, stats)))


def solution(mesh):
    return jax.shard_map(
        on_device, mesh=mesh, in_specs=(P(None, None, None, "tm", "space"),),
        out_specs=(P(None, ("space", "tm")), P()), check_vma=False)
```

```python
import jax
import jax.numpy as jnp
from jax import lax
from jax.experimental import pallas as pl
from jax.experimental.pallas import tpu as pltpu
from jax.sharding import PartitionSpec as P

MESH = pl.DeviceIdType.MESH
LANES = 128
NY = 8
NZ = 8
NCLASS = 4
NX = 4
NSPACE = 8
ROWS = 2
COORDS = 8
FAR_FIRST = (4, 3, 5, 2, 6, 1, 7)
Z_ORDER = (0, 7, 6, 1, 5, 2, 4, 3)
RELAYED = ((0, 4, 2, 0, (1,)), (0, 4, 6, 1, (0,)), (0, 5, 6, 0, (0, 1)), (7, 4, 5, 0, (0, 1)))
PAIRS = (2, 1, 3, 0)


def third_row(a, b):
    row = []
    for i, j in ((1, 2), (2, 0), (0, 1)):
        re = (a[i][0] * b[j][0] - a[i][1] * b[j][1]) - (a[j][0] * b[i][0] - a[j][1] * b[i][1])
        im = (a[j][0] * b[i][1] + a[j][1] * b[i][0]) - (a[i][0] * b[j][1] + a[i][1] * b[j][0])
        row.append((re, im))
    return row


def product(a, b):
    return (a[0] * b[0] - a[1] * b[1], a[0] * b[1] + a[1] * b[0])


def conj_product(a, b):
    return (a[0] * b[0] + a[1] * b[1], a[0] * b[1] - a[1] * b[0])


def project(p):
    q = p[1] * p[1]
    for v in p[2:]:
        q = q + v * v
    below = p[0] < 0.0
    scale = jnp.where(below, 1.0 - p[0], 1.0) / jnp.where(below, jnp.maximum(q, 1e-20), 1.0 + p[0])
    return [jnp.where(below & (q < 1e-20), 1e-10, p[1]) * scale] + [v * scale for v in p[2:]]


def weight(x):
    n = x[0] * x[0]
    for v in x[1:]:
        n = n + v * v
    return 2.0 / (1.0 + n)


def lift(x):
    w = weight(x)
    return [w - 1.0] + [w * v for v in x]


def reflector(x):
    r = weight(x) / (1.0 + x[0] * x[0])
    return (r, r * x[0]), [(1.0, x[0]), (x[1], x[2]), (x[3], x[4])]


def coordinates(two):
    a, b = two
    x = project([v for pair in a for v in pair])
    h, u = reflector(x)
    parts = [conj_product(u[k], b[k]) for k in range(3)]
    k = conj_product(h, (parts[0][0] + parts[1][0] + parts[2][0], parts[0][1] + parts[1][1] + parts[2][1]))
    rest = []
    for j in (1, 2):
        off = product(u[j], k)
        rest += [b[j][0] - off[0], b[j][1] - off[1]]
    return x + project(rest)


def first_rows(v):
    x = v[:5]
    p = lift(x)
    q = lift(v[5:])
    h, u = reflector(x)
    one = conj_product(u[1], (q[0], q[1]))
    two = conj_product(u[2], (q[2], q[3]))
    g = product(h, (one[0] + two[0], one[1] + two[1]))
    off = [product(g, u[k]) for k in range(3)]
    return [[(p[0], p[1]), (p[2], p[3]), (p[4], p[5])],
            [(-off[0][0], -off[0][1]), (q[0] - off[1][0], q[1] - off[1][1]), (q[2] - off[2][0], q[3] - off[2][1])]]


def times(left, right):
    out = []
    for row in left:
        new = []
        for c in range(3):
            re = im = None
            for k in range(3):
                lr, li = row[k]
                rr, ri = right[k][c]
                tr = lr * rr - li * ri
                ti = lr * ri + li * rr
                re = tr if re is None else re + tr
                im = ti if im is None else im + ti
            new.append((re, im))
        out.append(new)
    return out


def full(two):
    return [two[0], two[1], third_row(two[0], two[1])]


def kernel(links, ploop_out, stats_out, lbuf, ysend, yvia, yrecv, ymat, zsend, zrecv, zmat, phold, prow, arecv, brecv,
           near_sem, load_sem, via_sem, vsend_sem, ysend_sem, yrecv_sem, zsend_sem, zrecv_sem, psend_sem, precv_sem,
           asend_sem, arecv_sem, bsend_sem, brecv_sem):
    tm = lax.axis_index("tm")
    s = lax.axis_index("space")
    z = lax.div(tm, NY)
    y = lax.rem(tm, NY)
    x = lax.div(s, 2)
    core = lax.rem(s, 2)

    def at(dz, dy, dx, to):
        return (lax.rem(z + dz + NZ, NZ) * NY + lax.rem(y + dy + NY, NY), lax.rem(x + dx, NX) * 2 + to)

    def tell(sem, whom):
        for where in whom:
            pl.semaphore_signal(sem, inc=1, device_id=where, device_id_type=MESH)

    def relayed(start, end):
        found = False
        for i, j in {(r[0], r[1]): 0 for r in RELAYED}:
            found = found | ((start == i) & (end == j))
        return found

    direct = NY - 1 - sum(jnp.where(y == i, 1, 0) for i, _ in {(r[0], r[1]): 0 for r in RELAYED})
    near = [at(1, 0, 0, 1), at(-1, 0, 0, 1), at(0, 0, 1, 1), at(0, 0, 3, 1)]
    farther = [at(2, 0, 0, 1), at(-2, 0, 0, 1), at(0, 0, 2, 1)]
    barrier = pltpu.get_barrier_semaphore()

    @pl.when(core == 1)
    def _():
        for d in FAR_FIRST:
            @pl.when(jnp.logical_not(relayed(lax.rem(y + d, NY), y)))
            def _():
                tell(barrier, [at(0, d, 0, 1), at(0, d, 0, 0)])

        tell(barrier, near + [at(0, 0, 0, 0)])

    @pl.when(core == 0)
    def _():
        tell(barrier, [at(0, 0, 0, 1)])

    pairs = [lax.rem(lax.div(y, 2) + step, 4) for step in PAIRS]
    for k, m in enumerate(pairs):
        for t in range(4):
            pltpu.make_async_copy(links.at[:, :, m, t], lbuf.at[k, t], load_sem.at[k]).start()

    def local(k):
        pltpu.make_async_copy(lbuf.at[k], lbuf.at[k], load_sem.at[k]).wait()

        def matrix(t, rows):
            return [[(lbuf[k, t, r * 3 + c], lbuf[k, t, 9 + r * 3 + c]) for c in range(3)]
                    for r in range(rows)]

        acc = matrix(0, ROWS)
        for t in range(1, 4):
            acc = times(acc, matrix(t, 3))
        for i, v in enumerate(coordinates(acc)):
            for h in range(2):
                ysend[pairs[k] * 2 + h, i] = v[4 * h:4 * h + 4]

    def ycopy(q):
        pltpu.make_async_remote_copy(
            src_ref=ysend.at[q], dst_ref=yrecv.at[y, :, pl.ds(pl.multiple_of(core * NCLASS, NCLASS), NCLASS)],
            send_sem=ysend_sem, recv_sem=yrecv_sem.at[y, core], device_id=(z * NY + q, x * 2 + 1), device_id_type=MESH).start()

    for k in range(4):
        local(k)
        if k == 0:
            pl.semaphore_wait(barrier, jnp.where(core == 1, direct + len(near) + 1, direct + 1))

            @pl.when(core == 1)
            def _():
                tell(near_sem.at[0], near)

        for start, end, by, slot, cores in RELAYED:
            if k == (2 if start == 7 else 0):
                @pl.when((y == start) & ((core == cores[0]) | (core == cores[-1])))
                def _():
                    pltpu.make_async_remote_copy(
                        src_ref=ysend.at[end], dst_ref=yvia.at[slot, core], send_sem=ysend_sem,
                        recv_sem=via_sem.at[slot, core], device_id=(z * NY + by, x * 2 + 1),
                        device_id_type=MESH).start()

        for h in range(2):
            q = pairs[k] * 2 + h

            @pl.when(jnp.logical_not(relayed(y, q)) & ((q != y) | (core == 0)))
            def _():
                ycopy(q)

    def store(ref, j, mat):
        for r in range(3):
            for c in range(3):
                for p in range(2):
                    ref[j, (r * 3 + c) * 2 + p] = mat[r][c][p]

    def load(ref, j):
        return [[(ref[j, (r * 3 + c) * 2], ref[j, (r * 3 + c) * 2 + 1]) for c in range(3)] for r in range(3)]

    def sent(ref, sem):
        pltpu.make_async_remote_copy(
            src_ref=ref, dst_ref=ref, send_sem=sem, recv_sem=sem,
            device_id=at(0, 0, 0, 1 - core), device_id_type=MESH).wait_send()

    def arrived(ref, sem):
        pltpu.make_async_copy(ref, ref, sem).wait()

    half = lax.rem(y, 2)
    holder = lax.div(z, NCLASS) == half
    lane = lax.broadcasted_iota(jnp.int32, (1, LANES), 1)

    @pl.when(core == 0)
    def _():
        arrived(prow, precv_sem)
        arrived(brecv, brecv_sem)
        sent(ysend, ysend_sem)

    @pl.when(core == 1)
    def _():
        yrecv[y, :, NCLASS:] = ysend[y]
        pl.semaphore_wait(near_sem.at[0], len(near))
        tell(near_sem.at[1], farther)

        for start, end, by, slot, cores in RELAYED:
            @pl.when(y == by)
            def _():
                for to in cores:
                    arrived(yvia.at[slot, to], via_sem.at[slot, to])
                    pltpu.make_async_remote_copy(
                        src_ref=yvia.at[slot, to], dst_ref=yrecv.at[start, :, pl.ds(NCLASS * to, NCLASS)],
                        send_sem=vsend_sem, recv_sem=yrecv_sem.at[start, to], device_id=(z * NY + end, s),
                        device_id_type=MESH).start()

        for d in FAR_FIRST + (0,):
            j = lax.rem(y + d, NY)
            arrived(yrecv.at[j, :, pl.ds(0, NCLASS)], yrecv_sem.at[j, 0])
            if d != 0:
                arrived(yrecv.at[j, :, pl.ds(NCLASS, NCLASS)], yrecv_sem.at[j, 1])
            store(ymat, j, full(first_rows([yrecv[j, i] for i in range(COORDS)])))
        acc = load(ymat, 0)[:ROWS]
        for j in range(1, NY):
            acc = times(acc, load(ymat, j))
        for i, v in enumerate(coordinates(acc)):
            for k in range(NCLASS):
                for to in range(2):
                    row = NCLASS * to + k
                    at_row = k // 2 * 2 + to
                    zsend[i, k % 2, at_row:at_row + 1] = v[row:row + 1]

        pl.semaphore_wait(near_sem.at[1], len(farther))
        tell(near_sem.at[2], [at(0, 0, 2, 1)])
        odd = lax.rem(z, 2)
        for q in Z_ORDER:
            @pl.when(z != q)
            def _():
                pltpu.make_async_remote_copy(
                    src_ref=zsend.at[:, q % 2], dst_ref=zrecv.at[:, pl.ds(pl.multiple_of(z * 4, 4), 4)],
                    send_sem=zsend_sem, recv_sem=zrecv_sem, device_id=(q * NY + y, s), device_id_type=MESH).start()

        zrecv[:, pl.ds(pl.multiple_of(z * 4, 4), 4)] = zsend[:, odd]
        arrived(zrecv.at[:, pl.ds(0, 4 * NZ - 4)], zrecv_sem)

        for j in range(4):
            mat = full(first_rows([zrecv[i, 8 * j:8 * j + 8] for i in range(COORDS)]))
            for r in range(3):
                for c in range(3):
                    for p in range(2):
                        zmat[(r * 3 + c) * 2 + p, 8 * j:8 * j + 8] = mat[r][c][p]

        def slab(j):
            return [[tuple(zmat[(r * 3 + c) * 2 + p, 4 * j:4 * j + 4] for p in range(2)) for c in range(3)]
                    for r in range(3)]

        acc = slab(0)[:ROWS]
        for j in range(1, NZ):
            acc = times(acc, slab(j))
        whole = full(acc)
        re = (whole[0][0][0] + whole[1][1][0] + whole[2][2][0]) / 3.0
        im = (whole[0][0][1] + whole[1][1][1] + whole[2][2][1]) / 3.0

        def total(value):
            return jnp.sum(jnp.sum(value, axis=1, keepdims=True), axis=0, keepdims=True)

        sums = jnp.where(lane == 0, total(re), jnp.where(lane == 1, total(im), total(re * re + im * im)))
        arecv[y] = sums
        for d in FAR_FIRST:
            pltpu.make_async_remote_copy(
                src_ref=arecv.at[y], dst_ref=arecv.at[y], send_sem=asend_sem,
                recv_sem=arecv_sem, device_id=at(0, d, 0, 1), device_id_type=MESH).start()

        @pl.when(holder)
        def _():
            for to in range(2):
                for p, value in enumerate((re, im)):
                    phold[to, p:p + 1] = jnp.where(lax.rem(z, NCLASS) < 2, value[to:to + 1], value[2 + to:3 + to])
            other = 1 - 2 * half
            for to, where in ((0, (tm, s - 1)), (0, (tm + other, s - 1)), (1, (tm + other, s))):
                pltpu.make_async_remote_copy(
                    src_ref=phold.at[to], dst_ref=prow, send_sem=psend_sem, recv_sem=precv_sem,
                    device_id=where, device_id_type=MESH).start()
            prow[...] = phold[1]

        arrived(arecv.at[pl.ds(0, NY - 1)], arecv_sem)
        mine = odd * NX + x
        brecv[mine] = jnp.sum(arecv[...], axis=0)
        pl.semaphore_wait(near_sem.at[2], 1)
        for dz in (1, 0):
            for dx in (2, 1, 3, 0):
                for to in (0, 1):
                    if dz != 0 or dx != 0 or to == 0:
                        pltpu.make_async_remote_copy(
                            src_ref=brecv.at[mine], dst_ref=brecv.at[mine], send_sem=bsend_sem,
                            recv_sem=brecv_sem, device_id=at(dz, 0, dx, to), device_id_type=MESH).start()

        @pl.when(jnp.logical_not(holder))
        def _():
            arrived(prow, precv_sem)

        arrived(brecv.at[pl.ds(0, 2 * NX - 1)], brecv_sem)
        sent(ysend.at[pl.ds(0, NY - 1)], ysend_sem)
        for _, _, by, _, cores in RELAYED:
            @pl.when(y == by)
            def _():
                for _ in cores:
                    sent(yvia.at[0, 0], vsend_sem)

        sent(zrecv.at[:, pl.ds(0, 4 * NZ - 4)], zsend_sem)
        sent(arecv.at[pl.ds(0, NY - 1)], asend_sem)
        sent(brecv, bsend_sem)
        sent(brecv.at[pl.ds(0, 2 * NX - 1)], bsend_sem)

        @pl.when(holder)
        def _():
            for _ in range(3):
                sent(prow, psend_sem)

    ploop_out[...] = jnp.where(half == 0, prow[:, :64], prow[:, 64:])
    grand = jnp.sum(brecv[...], axis=0) / (NY * NCLASS * NSPACE * LANES)
    means = jnp.where(lane < 2, grand * grand, 0.0)
    stats = grand - jnp.where(lane == 2, jnp.sum(means, axis=1, keepdims=True), 0.0)
    stats_out[...] = stats[0, :3]


def finish(ploop_in, stats_in, ploop_out, stats_out, sems):
    copies = [pltpu.make_async_copy(ploop_in, ploop_out, sems.at[0]),
              pltpu.make_async_copy(stats_in, stats_out, sems.at[1])]
    for copy in copies:
        copy.start()
    for copy in copies:
        copy.wait()


def on_device(links):
    times_here, sites = links.shape[3:]
    rows = sites // LANES
    view = links.reshape(18, times_here, rows, LANES).transpose(0, 2, 1, 3)
    view = view.reshape(18, 8, 4, times_here, LANES)
    f32 = jnp.float32
    dma = pltpu.SemaphoreType.DMA
    vmem = pl.BlockSpec(memory_space=pltpu.VMEM)
    ploop, stats = pl.pallas_call(
        kernel,
        out_shape=(pltpu.VMEM((2, sites // 64), f32), pltpu.VMEM((3,), f32)),
        in_specs=[pl.BlockSpec(memory_space=pl.ANY)],
        out_specs=(vmem, vmem),
        scratch_shapes=[
            pltpu.VMEM((4, 4, 18, 8, LANES), f32),
            pltpu.VMEM((NY, COORDS, NCLASS, LANES), f32),
            pltpu.VMEM((2, 2, COORDS, NCLASS, LANES), f32),
            pltpu.VMEM((NY, COORDS, 2 * NCLASS, LANES), f32),
            pltpu.VMEM((NY, 18, 2 * NCLASS, LANES), f32),
            pltpu.VMEM((COORDS, 2, 4, LANES), f32),
            pltpu.VMEM((COORDS, 4 * NZ, LANES), f32),
            pltpu.VMEM((18, 4 * NZ, LANES), f32),
            pltpu.VMEM((2, 2, LANES), f32),
            pltpu.VMEM((2, LANES), f32),
            pltpu.VMEM((NY, 1, LANES), f32),
            pltpu.VMEM((2 * NX, 1, LANES), f32),
            pltpu.SemaphoreType.REGULAR((3,)),
            dma((4,)), dma((2, 2)), dma, dma, dma((NY, 2)), dma, dma, dma, dma, dma, dma, dma, dma,
        ],
        compiler_params=pltpu.CompilerParams(collective_id=0, has_side_effects=True),
    )(view)
    hbm = pl.BlockSpec(memory_space=pl.ANY)
    return pl.pallas_call(
        finish,
        out_shape=(jax.ShapeDtypeStruct((2, sites // 64), f32), jax.ShapeDtypeStruct((3,), f32)),
        in_specs=[vmem, vmem],
        out_specs=(hbm, hbm),
        scratch_shapes=[dma((2,))],
    )(*(pltpu.with_memory_space_constraint(x, pltpu.VMEM) for x in (ploop, stats)))


def solution(mesh):
    return jax.shard_map(
        on_device, mesh=mesh, in_specs=(P(None, None, None, "tm", "space"),),
        out_specs=(P(None, ("space", "tm")), P()), check_vma=False)
```

```python
import jax
import jax.numpy as jnp
from jax import lax
from jax.experimental import pallas as pl
from jax.experimental.pallas import tpu as pltpu
from jax.sharding import PartitionSpec as P

MESH = pl.DeviceIdType.MESH
LANES = 128
NY = 8
NZ = 8
NCLASS = 4
NX = 4
NSPACE = 8
ROWS = 2
COORDS = 8
FAR_FIRST = (4, 3, 5, 2, 6, 1, 7)
Z_ORDER = (0, 7, 6, 1, 5, 2, 4, 3)
SUM_ORDER = (0, 1, 7, 2, 6, 3, 5, 4)
RELAYED = ((0, 4, 2, 0, (1,)), (0, 4, 6, 1, (0,)), (0, 5, 6, 0, (0, 1)), (7, 4, 5, 0, (0, 1)))
PAIRS = (2, 1, 3, 0)


def third_row(a, b):
    row = []
    for i, j in ((1, 2), (2, 0), (0, 1)):
        re = (a[i][0] * b[j][0] - a[i][1] * b[j][1]) - (a[j][0] * b[i][0] - a[j][1] * b[i][1])
        im = (a[j][0] * b[i][1] + a[j][1] * b[i][0]) - (a[i][0] * b[j][1] + a[i][1] * b[j][0])
        row.append((re, im))
    return row


def product(a, b):
    return (a[0] * b[0] - a[1] * b[1], a[0] * b[1] + a[1] * b[0])


def conj_product(a, b):
    return (a[0] * b[0] + a[1] * b[1], a[0] * b[1] - a[1] * b[0])


def project(p):
    q = p[1] * p[1]
    for v in p[2:]:
        q = q + v * v
    below = p[0] < 0.0
    scale = jnp.where(below, 1.0 - p[0], 1.0) / jnp.where(below, jnp.maximum(q, 1e-20), 1.0 + p[0])
    return [jnp.where(below & (q < 1e-20), 1e-10, p[1]) * scale] + [v * scale for v in p[2:]]


def weight(x):
    n = x[0] * x[0]
    for v in x[1:]:
        n = n + v * v
    return 2.0 / (1.0 + n)


def lift(x):
    w = weight(x)
    return [w - 1.0] + [w * v for v in x]


def reflector(x):
    r = weight(x) / (1.0 + x[0] * x[0])
    return (r, r * x[0]), [(1.0, x[0]), (x[1], x[2]), (x[3], x[4])]


def coordinates(two):
    a, b = two
    x = project([v for pair in a for v in pair])
    h, u = reflector(x)
    parts = [conj_product(u[k], b[k]) for k in range(3)]
    k = conj_product(h, (parts[0][0] + parts[1][0] + parts[2][0], parts[0][1] + parts[1][1] + parts[2][1]))
    rest = []
    for j in (1, 2):
        off = product(u[j], k)
        rest += [b[j][0] - off[0], b[j][1] - off[1]]
    return x + project(rest)


def first_rows(v):
    x = v[:5]
    p = lift(x)
    q = lift(v[5:])
    h, u = reflector(x)
    one = conj_product(u[1], (q[0], q[1]))
    two = conj_product(u[2], (q[2], q[3]))
    g = product(h, (one[0] + two[0], one[1] + two[1]))
    off = [product(g, u[k]) for k in range(3)]
    return [[(p[0], p[1]), (p[2], p[3]), (p[4], p[5])],
            [(-off[0][0], -off[0][1]), (q[0] - off[1][0], q[1] - off[1][1]), (q[2] - off[2][0], q[3] - off[2][1])]]


def times(left, right):
    out = []
    for row in left:
        new = []
        for c in range(3):
            re = im = None
            for k in range(3):
                lr, li = row[k]
                rr, ri = right[k][c]
                tr = lr * rr - li * ri
                ti = lr * ri + li * rr
                re = tr if re is None else re + tr
                im = ti if im is None else im + ti
            new.append((re, im))
        out.append(new)
    return out


def full(two):
    return [two[0], two[1], third_row(two[0], two[1])]


def kernel(links, ploop_out, stats_out, lbuf, ysend, yvia, yrecv, ymat, zsend, zrecv, zmat, phold, prow, srow, rows,
           near_sem, load_sem, via_sem, vsend_sem, ysend_sem, yrecv_sem, zsend_sem, zrecv_sem, psend_sem, precv_sem,
           asend_sem, arecv_sem):
    tm = lax.axis_index("tm")
    s = lax.axis_index("space")
    z = lax.div(tm, NY)
    y = lax.rem(tm, NY)
    x = lax.div(s, 2)
    core = lax.rem(s, 2)

    def at(dz, dy, dx, to):
        return (lax.rem(z + dz + NZ, NZ) * NY + lax.rem(y + dy + NY, NY), lax.rem(x + dx, NX) * 2 + to)

    def tell(sem, whom):
        for where in whom:
            pl.semaphore_signal(sem, inc=1, device_id=where, device_id_type=MESH)

    def relayed(start, end):
        found = False
        for i, j in {(r[0], r[1]): 0 for r in RELAYED}:
            found = found | ((start == i) & (end == j))
        return found

    direct = NY - 1 - sum(jnp.where(y == i, 1, 0) for i, _ in {(r[0], r[1]): 0 for r in RELAYED})
    near = [at(1, 0, 0, 1), at(-1, 0, 0, 1), at(0, 0, 1, 1), at(0, 0, 3, 1)]
    farther = [at(2, 0, 0, 1), at(-2, 0, 0, 1), at(0, 0, 2, 1)]
    barrier = pltpu.get_barrier_semaphore()

    @pl.when(core == 1)
    def _():
        for d in FAR_FIRST:
            @pl.when(jnp.logical_not(relayed(lax.rem(y + d, NY), y)))
            def _():
                tell(barrier, [at(0, d, 0, 1), at(0, d, 0, 0)])

        tell(barrier, near + [at(0, 0, 0, 0)])

    @pl.when(core == 0)
    def _():
        tell(barrier, [at(0, 0, 0, 1)])

    pairs = PAIRS
    for k, m in enumerate(pairs):
        for t in range(4):
            pltpu.make_async_copy(links.at[:, :, m, t], lbuf.at[k, t], load_sem.at[k]).start()

    def local(k):
        pltpu.make_async_copy(lbuf.at[k], lbuf.at[k], load_sem.at[k]).wait()

        def matrix(t, rows):
            return [[(lbuf[k, t, r * 3 + c], lbuf[k, t, 9 + r * 3 + c]) for c in range(3)]
                    for r in range(rows)]

        acc = matrix(0, ROWS)
        for t in range(1, 4):
            acc = times(acc, matrix(t, 3))
        for i, v in enumerate(coordinates(acc)):
            for h in range(2):
                ysend[pairs[k] * 2 + h, i] = v[4 * h:4 * h + 4]

    def ycopy(q):
        pltpu.make_async_remote_copy(
            src_ref=ysend.at[q], dst_ref=yrecv.at[y, :, pl.ds(pl.multiple_of(core * NCLASS, NCLASS), NCLASS)],
            send_sem=ysend_sem, recv_sem=yrecv_sem.at[y, core], device_id=(z * NY + q, x * 2 + 1), device_id_type=MESH).start()

    for k in range(4):
        local(k)
        if k == 0:
            pl.semaphore_wait(barrier, jnp.where(core == 1, direct + len(near) + 1, direct + 1))

            @pl.when(core == 1)
            def _():
                tell(near_sem.at[0], near)

        for start, end, by, slot, cores in RELAYED:
            if k == 0:
                @pl.when((y == start) & ((core == cores[0]) | (core == cores[-1])))
                def _():
                    pltpu.make_async_remote_copy(
                        src_ref=ysend.at[end], dst_ref=yvia.at[slot, core], send_sem=ysend_sem,
                        recv_sem=via_sem.at[slot, core], device_id=(z * NY + by, x * 2 + 1),
                        device_id_type=MESH).start()

        for h in range(2):
            q = pairs[k] * 2 + h

            @pl.when(jnp.logical_not(relayed(y, q)) & ((q != y) | (core == 0)))
            def _():
                ycopy(q)

    def store(ref, j, mat):
        for r in range(3):
            for c in range(3):
                for p in range(2):
                    ref[j, (r * 3 + c) * 2 + p] = mat[r][c][p]

    def load(ref, j):
        return [[(ref[j, (r * 3 + c) * 2], ref[j, (r * 3 + c) * 2 + 1]) for c in range(3)] for r in range(3)]

    def sent(ref, sem):
        pltpu.make_async_remote_copy(
            src_ref=ref, dst_ref=ref, send_sem=sem, recv_sem=sem,
            device_id=at(0, 0, 0, 1 - core), device_id_type=MESH).wait_send()

    def arrived(ref, sem):
        pltpu.make_async_copy(ref, ref, sem).wait()

    half = lax.rem(y, 2)
    holder = lax.div(z, NCLASS) == half
    lane = lax.broadcasted_iota(jnp.int32, (1, LANES), 1)

    @pl.when(core == 0)
    def _():
        arrived(prow, precv_sem)
        arrived(rows, arecv_sem)
        sent(ysend, ysend_sem)

    @pl.when(core == 1)
    def _():
        yrecv[y, :, NCLASS:] = ysend[y]
        pl.semaphore_wait(near_sem.at[0], len(near))
        tell(near_sem.at[1], farther)

        for start, end, by, slot, cores in RELAYED:
            @pl.when(y == by)
            def _():
                for to in cores:
                    arrived(yvia.at[slot, to], via_sem.at[slot, to])
                    pltpu.make_async_remote_copy(
                        src_ref=yvia.at[slot, to], dst_ref=yrecv.at[start, :, pl.ds(NCLASS * to, NCLASS)],
                        send_sem=vsend_sem, recv_sem=yrecv_sem.at[start, to], device_id=(z * NY + end, s),
                        device_id_type=MESH).start()

        for d in FAR_FIRST + (0,):
            j = lax.rem(y + d, NY)
            arrived(yrecv.at[j, :, pl.ds(0, NCLASS)], yrecv_sem.at[j, 0])
            if d != 0:
                arrived(yrecv.at[j, :, pl.ds(NCLASS, NCLASS)], yrecv_sem.at[j, 1])
            store(ymat, j, full(first_rows([yrecv[j, i] for i in range(COORDS)])))
        acc = load(ymat, 0)[:ROWS]
        for j in range(1, NY):
            acc = times(acc, load(ymat, j))
        for i, v in enumerate(coordinates(acc)):
            for k in range(NCLASS):
                for to in range(2):
                    row = NCLASS * to + k
                    at_row = k // 2 * 2 + to
                    zsend[i, k % 2, at_row:at_row + 1] = v[row:row + 1]

        pl.semaphore_wait(near_sem.at[1], len(farther))
        tell(near_sem.at[2], [at(0, 0, dx, 1) for dx in (2, 1, 3)] + [at(-1, 0, dx, 1) for dx in range(NX)])
        odd = lax.rem(z, 2)
        for q in Z_ORDER:
            @pl.when(z != q)
            def _():
                pltpu.make_async_remote_copy(
                    src_ref=zsend.at[:, q % 2], dst_ref=zrecv.at[:, pl.ds(pl.multiple_of(z * 4, 4), 4)],
                    send_sem=zsend_sem, recv_sem=zrecv_sem, device_id=(q * NY + y, s), device_id_type=MESH).start()

        zrecv[:, pl.ds(pl.multiple_of(z * 4, 4), 4)] = zsend[:, odd]
        arrived(zrecv.at[:, pl.ds(0, 4 * NZ - 4)], zrecv_sem)

        for j in range(4):
            mat = full(first_rows([zrecv[i, 8 * j:8 * j + 8] for i in range(COORDS)]))
            for r in range(3):
                for c in range(3):
                    for p in range(2):
                        zmat[(r * 3 + c) * 2 + p, 8 * j:8 * j + 8] = mat[r][c][p]

        def slab(j):
            return [[tuple(zmat[(r * 3 + c) * 2 + p, 4 * j:4 * j + 4] for p in range(2)) for c in range(3)]
                    for r in range(3)]

        acc = slab(0)[:ROWS]
        for j in range(1, NZ):
            acc = times(acc, slab(j))
        whole = full(acc)
        re = (whole[0][0][0] + whole[1][1][0] + whole[2][2][0]) / 3.0
        im = (whole[0][0][1] + whole[1][1][1] + whole[2][2][1]) / 3.0

        def total(value):
            return jnp.sum(jnp.sum(value, axis=1, keepdims=True), axis=0, keepdims=True)

        sums = jnp.where(lane == 0, total(re), jnp.where(lane == 1, total(im), total(re * re + im * im)))
        mine = (odd * NX + x) * NY + y
        srow[...] = sums
        pl.semaphore_wait(near_sem.at[2], 2 * NX - 1)
        last = z == NZ - 1
        for step in (0, 1):
            dz = jnp.where(last, 1 - step, step)
            for q in SUM_ORDER:
                for dx in (2, 1, 3, 0):
                    for to in (1, 0):
                        def send():
                            pltpu.make_async_remote_copy(
                                src_ref=srow, dst_ref=rows.at[pl.ds(mine, 1)], send_sem=asend_sem, recv_sem=arecv_sem,
                                device_id=(lax.rem(z + dz, NZ) * NY + q, lax.rem(x + dx, NX) * 2 + to),
                                device_id_type=MESH).start()

                        if dx == 0 and to == 1:
                            pl.when((dz != 0) | (y != q))(send)
                        else:
                            send()

        rows[pl.ds(mine, 1)] = sums
        @pl.when(holder)
        def _():
            for to in range(2):
                for p, value in enumerate((re, im)):
                    phold[to, p:p + 1] = jnp.where(lax.rem(z, NCLASS) < 2, value[to:to + 1], value[2 + to:3 + to])
            other = 1 - 2 * half
            for to, where in ((0, (tm, s - 1)), (0, (tm + other, s - 1)), (1, (tm + other, s))):
                pltpu.make_async_remote_copy(
                    src_ref=phold.at[to], dst_ref=prow, send_sem=psend_sem, recv_sem=precv_sem,
                    device_id=where, device_id_type=MESH).start()
            prow[...] = phold[1]

        @pl.when(jnp.logical_not(holder))
        def _():
            arrived(prow, precv_sem)

        arrived(rows.at[pl.ds(0, 2 * NX * NY - 1)], arecv_sem)
        sent(ysend.at[pl.ds(0, NY - 1)], ysend_sem)
        for _, _, by, _, cores in RELAYED:
            @pl.when(y == by)
            def _():
                for _ in cores:
                    sent(yvia.at[0, 0], vsend_sem)

        sent(zrecv.at[:, pl.ds(0, 4 * NZ - 4)], zsend_sem)
        sent(rows, asend_sem)
        sent(rows.at[pl.ds(0, 2 * NX * NY - 1)], asend_sem)

        @pl.when(holder)
        def _():
            for _ in range(3):
                sent(prow, psend_sem)

    ploop_out[...] = jnp.where(half == 0, prow[:, :64], prow[:, 64:])
    grand = jnp.sum(rows[...], axis=0, keepdims=True) / (NY * NCLASS * NSPACE * LANES)
    means = jnp.where(lane < 2, grand * grand, 0.0)
    stats = grand - jnp.where(lane == 2, jnp.sum(means, axis=1, keepdims=True), 0.0)
    stats_out[...] = stats[0, :3]


def finish(ploop_in, stats_in, ploop_out, stats_out, sems):
    copies = [pltpu.make_async_copy(ploop_in, ploop_out, sems.at[0]),
              pltpu.make_async_copy(stats_in, stats_out, sems.at[1])]
    for copy in copies:
        copy.start()
    for copy in copies:
        copy.wait()


def on_device(links):
    times_here, sites = links.shape[3:]
    rows = sites // LANES
    view = links.reshape(18, times_here, rows, LANES).transpose(0, 2, 1, 3)
    view = view.reshape(18, 8, 4, times_here, LANES)
    f32 = jnp.float32
    dma = pltpu.SemaphoreType.DMA
    vmem = pl.BlockSpec(memory_space=pltpu.VMEM)
    ploop, stats = pl.pallas_call(
        kernel,
        out_shape=(pltpu.VMEM((2, sites // 64), f32), pltpu.VMEM((3,), f32)),
        in_specs=[pl.BlockSpec(memory_space=pl.ANY)],
        out_specs=(vmem, vmem),
        scratch_shapes=[
            pltpu.VMEM((4, 4, 18, 8, LANES), f32),
            pltpu.VMEM((NY, COORDS, NCLASS, LANES), f32),
            pltpu.VMEM((2, 2, COORDS, NCLASS, LANES), f32),
            pltpu.VMEM((NY, COORDS, 2 * NCLASS, LANES), f32),
            pltpu.VMEM((NY, 18, 2 * NCLASS, LANES), f32),
            pltpu.VMEM((COORDS, 2, 4, LANES), f32),
            pltpu.VMEM((COORDS, 4 * NZ, LANES), f32),
            pltpu.VMEM((18, 4 * NZ, LANES), f32),
            pltpu.VMEM((2, 2, LANES), f32),
            pltpu.VMEM((2, LANES), f32),
            pltpu.VMEM((1, LANES), f32),
            pltpu.VMEM((2 * NX * NY, LANES), f32),
            pltpu.SemaphoreType.REGULAR((3,)),
            dma((4,)), dma((2, 2)), dma, dma, dma((NY, 2)), dma, dma, dma, dma, dma, dma,
        ],
        compiler_params=pltpu.CompilerParams(collective_id=0, has_side_effects=True),
    )(view)
    hbm = pl.BlockSpec(memory_space=pl.ANY)
    return pl.pallas_call(
        finish,
        out_shape=(jax.ShapeDtypeStruct((2, sites // 64), f32), jax.ShapeDtypeStruct((3,), f32)),
        in_specs=[vmem, vmem],
        out_specs=(hbm, hbm),
        scratch_shapes=[dma((2,))],
    )(*(pltpu.with_memory_space_constraint(x, pltpu.VMEM) for x in (ploop, stats)))


def solution(mesh):
    return jax.shard_map(
        on_device, mesh=mesh, in_specs=(P(None, None, None, "tm", "space"),),
        out_specs=(P(None, ("space", "tm")), P()), check_vma=False)
```

```python
import jax
import jax.numpy as jnp
from jax import lax
from jax.experimental import pallas as pl
from jax.experimental.pallas import tpu as pltpu
from jax.sharding import PartitionSpec as P

MESH = pl.DeviceIdType.MESH
LANES = 128
NY = 8
NZ = 8
NCLASS = 4
NX = 4
NSPACE = 8
ROWS = 2
COORDS = 8
FAR_FIRST = (4, 3, 5, 2, 6, 1, 7)
Z_ORDER = (0, 7, 6, 1, 5, 2, 4, 3)
EARLY = 3
PASS_ON = ((2, (3, 4, 5, 6, 7)),)
SUM_ORDER = (0, 1, 7, 2, 6, 3, 5, 4)
RELAYED = ((0, 4, 2, 0, (1,)), (0, 4, 6, 1, (0,)), (0, 5, 6, 0, (0, 1)), (7, 4, 5, 0, (0, 1)))
PAIRS = (2, 1, 3, 0)


def third_row(a, b):
    row = []
    for i, j in ((1, 2), (2, 0), (0, 1)):
        re = (a[i][0] * b[j][0] - a[i][1] * b[j][1]) - (a[j][0] * b[i][0] - a[j][1] * b[i][1])
        im = (a[j][0] * b[i][1] + a[j][1] * b[i][0]) - (a[i][0] * b[j][1] + a[i][1] * b[j][0])
        row.append((re, im))
    return row


def product(a, b):
    return (a[0] * b[0] - a[1] * b[1], a[0] * b[1] + a[1] * b[0])


def conj_product(a, b):
    return (a[0] * b[0] + a[1] * b[1], a[0] * b[1] - a[1] * b[0])


def project(p):
    q = p[1] * p[1]
    for v in p[2:]:
        q = q + v * v
    below = p[0] < 0.0
    scale = jnp.where(below, 1.0 - p[0], 1.0) / jnp.where(below, jnp.maximum(q, 1e-20), 1.0 + p[0])
    return [jnp.where(below & (q < 1e-20), 1e-10, p[1]) * scale] + [v * scale for v in p[2:]]


def weight(x):
    n = x[0] * x[0]
    for v in x[1:]:
        n = n + v * v
    return 2.0 / (1.0 + n)


def lift(x):
    w = weight(x)
    return [w - 1.0] + [w * v for v in x]


def reflector(x):
    r = weight(x) / (1.0 + x[0] * x[0])
    return (r, r * x[0]), [(1.0, x[0]), (x[1], x[2]), (x[3], x[4])]


def coordinates(two):
    a, b = two
    x = project([v for pair in a for v in pair])
    h, u = reflector(x)
    parts = [conj_product(u[k], b[k]) for k in range(3)]
    k = conj_product(h, (parts[0][0] + parts[1][0] + parts[2][0], parts[0][1] + parts[1][1] + parts[2][1]))
    rest = []
    for j in (1, 2):
        off = product(u[j], k)
        rest += [b[j][0] - off[0], b[j][1] - off[1]]
    return x + project(rest)


def first_rows(v):
    x = v[:5]
    p = lift(x)
    q = lift(v[5:])
    h, u = reflector(x)
    one = conj_product(u[1], (q[0], q[1]))
    two = conj_product(u[2], (q[2], q[3]))
    g = product(h, (one[0] + two[0], one[1] + two[1]))
    off = [product(g, u[k]) for k in range(3)]
    return [[(p[0], p[1]), (p[2], p[3]), (p[4], p[5])],
            [(-off[0][0], -off[0][1]), (q[0] - off[1][0], q[1] - off[1][1]), (q[2] - off[2][0], q[3] - off[2][1])]]


def times(left, right):
    out = []
    for row in left:
        new = []
        for c in range(3):
            re = im = None
            for k in range(3):
                lr, li = row[k]
                rr, ri = right[k][c]
                tr = lr * rr - li * ri
                ti = lr * ri + li * rr
                re = tr if re is None else re + tr
                im = ti if im is None else im + ti
            new.append((re, im))
        out.append(new)
    return out


def full(two):
    return [two[0], two[1], third_row(two[0], two[1])]


def kernel(links, ploop_out, stats_out, lbuf, ysend, yvia, yrecv, ymat, zsend, zrecv, zmat, phold, prow, srow, rows, final,
           near_sem, load_sem, via_sem, vsend_sem, ysend_sem, yrecv_sem, zsend_sem, zrecv_sem, psend_sem, precv_sem,
           asend_sem, arecv_sem, gsend_sem, grecv_sem):
    tm = lax.axis_index("tm")
    s = lax.axis_index("space")
    z = lax.div(tm, NY)
    y = lax.rem(tm, NY)
    x = lax.div(s, 2)
    core = lax.rem(s, 2)

    def at(dz, dy, dx, to):
        return (lax.rem(z + dz + NZ, NZ) * NY + lax.rem(y + dy + NY, NY), lax.rem(x + dx, NX) * 2 + to)

    def tell(sem, whom):
        for where in whom:
            pl.semaphore_signal(sem, inc=1, device_id=where, device_id_type=MESH)

    def relayed(start, end):
        found = False
        for i, j in {(r[0], r[1]): 0 for r in RELAYED}:
            found = found | ((start == i) & (end == j))
        return found

    direct = NY - 1 - sum(jnp.where(y == i, 1, 0) for i, _ in {(r[0], r[1]): 0 for r in RELAYED})
    near = [at(1, 0, 0, 1), at(-1, 0, 0, 1), at(0, 0, 1, 1), at(0, 0, 3, 1)]
    farther = [at(2, 0, 0, 1), at(-2, 0, 0, 1), at(0, 0, 2, 1)]
    barrier = pltpu.get_barrier_semaphore()

    @pl.when(core == 1)
    def _():
        for d in FAR_FIRST:
            @pl.when(jnp.logical_not(relayed(lax.rem(y + d, NY), y)))
            def _():
                tell(barrier, [at(0, d, 0, 1), at(0, d, 0, 0)])

        tell(barrier, near + [at(0, 0, 0, 0)])

    @pl.when(core == 0)
    def _():
        tell(barrier, [at(0, 0, 0, 1)])

    pairs = PAIRS
    for k, m in enumerate(pairs):
        for t in range(4):
            pltpu.make_async_copy(links.at[:, :, m, t], lbuf.at[k, t], load_sem.at[k]).start()

    def local(k):
        pltpu.make_async_copy(lbuf.at[k], lbuf.at[k], load_sem.at[k]).wait()

        def matrix(t, rows):
            return [[(lbuf[k, t, r * 3 + c], lbuf[k, t, 9 + r * 3 + c]) for c in range(3)]
                    for r in range(rows)]

        acc = matrix(0, ROWS)
        for t in range(1, 4):
            acc = times(acc, matrix(t, 3))
        for i, v in enumerate(coordinates(acc)):
            for h in range(2):
                ysend[pairs[k] * 2 + h, i] = v[4 * h:4 * h + 4]

    def ycopy(q):
        pltpu.make_async_remote_copy(
            src_ref=ysend.at[q], dst_ref=yrecv.at[y, :, pl.ds(pl.multiple_of(core * NCLASS, NCLASS), NCLASS)],
            send_sem=ysend_sem, recv_sem=yrecv_sem.at[y, core], device_id=(z * NY + q, x * 2 + 1), device_id_type=MESH).start()

    for k in range(4):
        local(k)
        if k == 0:
            pl.semaphore_wait(barrier, jnp.where(core == 1, direct + len(near) + 1, direct + 1))

            @pl.when(core == 1)
            def _():
                tell(near_sem.at[0], near)

        for start, end, by, slot, cores in RELAYED:
            if k == 0:
                @pl.when((y == start) & ((core == cores[0]) | (core == cores[-1])))
                def _():
                    pltpu.make_async_remote_copy(
                        src_ref=ysend.at[end], dst_ref=yvia.at[slot, core], send_sem=ysend_sem,
                        recv_sem=via_sem.at[slot, core], device_id=(z * NY + by, x * 2 + 1),
                        device_id_type=MESH).start()

        for h in range(2):
            q = pairs[k] * 2 + h

            @pl.when(jnp.logical_not(relayed(y, q)) & ((q != y) | (core == 0)))
            def _():
                ycopy(q)

    def store(ref, j, mat):
        for r in range(3):
            for c in range(3):
                for p in range(2):
                    ref[j, (r * 3 + c) * 2 + p] = mat[r][c][p]

    def load(ref, j):
        return [[(ref[j, (r * 3 + c) * 2], ref[j, (r * 3 + c) * 2 + 1]) for c in range(3)] for r in range(3)]

    def sent(ref, sem):
        pltpu.make_async_remote_copy(
            src_ref=ref, dst_ref=ref, send_sem=sem, recv_sem=sem,
            device_id=at(0, 0, 0, 1 - core), device_id_type=MESH).wait_send()

    def arrived(ref, sem):
        pltpu.make_async_copy(ref, ref, sem).wait()

    half = lax.rem(y, 2)
    holder = lax.div(z, NCLASS) == half
    lane = lax.broadcasted_iota(jnp.int32, (1, LANES), 1)

    @pl.when(core == 0)
    def _():
        arrived(prow, precv_sem)
        pl.when(z < EARLY)(lambda: arrived(rows, arecv_sem))
        pl.when(z >= EARLY)(lambda: arrived(final, grecv_sem))
        sent(ysend, ysend_sem)

    @pl.when(core == 1)
    def _():
        yrecv[y, :, NCLASS:] = ysend[y]
        pl.semaphore_wait(near_sem.at[0], len(near))
        tell(near_sem.at[1], farther)

        for start, end, by, slot, cores in RELAYED:
            @pl.when(y == by)
            def _():
                for to in cores:
                    arrived(yvia.at[slot, to], via_sem.at[slot, to])
                    pltpu.make_async_remote_copy(
                        src_ref=yvia.at[slot, to], dst_ref=yrecv.at[start, :, pl.ds(NCLASS * to, NCLASS)],
                        send_sem=vsend_sem, recv_sem=yrecv_sem.at[start, to], device_id=(z * NY + end, s),
                        device_id_type=MESH).start()

        for d in FAR_FIRST + (0,):
            j = lax.rem(y + d, NY)
            arrived(yrecv.at[j, :, pl.ds(0, NCLASS)], yrecv_sem.at[j, 0])
            if d != 0:
                arrived(yrecv.at[j, :, pl.ds(NCLASS, NCLASS)], yrecv_sem.at[j, 1])
            store(ymat, j, full(first_rows([yrecv[j, i] for i in range(COORDS)])))
        acc = load(ymat, 0)[:ROWS]
        for j in range(1, NY):
            acc = times(acc, load(ymat, j))
        for i, v in enumerate(coordinates(acc)):
            for k in range(NCLASS):
                for to in range(2):
                    row = NCLASS * to + k
                    at_row = k // 2 * 2 + to
                    zsend[i, k % 2, at_row:at_row + 1] = v[row:row + 1]

        pl.semaphore_wait(near_sem.at[1], len(farther))
        tell(near_sem.at[2], [at(0, 0, dx, 1) for dx in (2, 1, 3)] + [at(-1, 0, dx, 1) for dx in range(NX)])
        odd = lax.rem(z, 2)
        for q in Z_ORDER:
            @pl.when(z != q)
            def _():
                pltpu.make_async_remote_copy(
                    src_ref=zsend.at[:, q % 2], dst_ref=zrecv.at[:, pl.ds(pl.multiple_of(z * 4, 4), 4)],
                    send_sem=zsend_sem, recv_sem=zrecv_sem, device_id=(q * NY + y, s), device_id_type=MESH).start()

        zrecv[:, pl.ds(pl.multiple_of(z * 4, 4), 4)] = zsend[:, odd]
        arrived(zrecv.at[:, pl.ds(0, 4 * NZ - 4)], zrecv_sem)

        for j in range(4):
            mat = full(first_rows([zrecv[i, 8 * j:8 * j + 8] for i in range(COORDS)]))
            for r in range(3):
                for c in range(3):
                    for p in range(2):
                        zmat[(r * 3 + c) * 2 + p, 8 * j:8 * j + 8] = mat[r][c][p]

        def slab(j):
            return [[tuple(zmat[(r * 3 + c) * 2 + p, 4 * j:4 * j + 4] for p in range(2)) for c in range(3)]
                    for r in range(3)]

        acc = slab(0)[:ROWS]
        for j in range(1, NZ):
            acc = times(acc, slab(j))
        whole = full(acc)
        re = (whole[0][0][0] + whole[1][1][0] + whole[2][2][0]) / 3.0
        im = (whole[0][0][1] + whole[1][1][1] + whole[2][2][1]) / 3.0

        def total(value):
            return jnp.sum(jnp.sum(value, axis=1, keepdims=True), axis=0, keepdims=True)

        sums = jnp.where(lane == 0, total(re), jnp.where(lane == 1, total(im), total(re * re + im * im)))
        mine = (odd * NX + x) * NY + y
        srow[...] = sums
        pl.semaphore_wait(near_sem.at[2], 2 * NX - 1)
        last = z == NZ - 1
        for step in (0, 1):
            dz = jnp.where(last, 1 - step, step)
            end = lax.rem(z + dz, NZ)

            @pl.when(end < EARLY)
            def _():
                for q in SUM_ORDER:
                    for dx in (2, 1, 3, 0):
                        for to in (1, 0):
                            def send():
                                pltpu.make_async_remote_copy(
                                    src_ref=srow, dst_ref=rows.at[pl.ds(mine, 1)], send_sem=asend_sem, recv_sem=arecv_sem,
                                    device_id=(end * NY + q, lax.rem(x + dx, NX) * 2 + to), device_id_type=MESH).start()

                            if dx == 0 and to == 1:
                                pl.when((dz != 0) | (y != q))(send)
                            else:
                                send()

        rows[pl.ds(mine, 1)] = sums
        @pl.when(holder)
        def _():
            for to in range(2):
                for p, value in enumerate((re, im)):
                    phold[to, p:p + 1] = jnp.where(lax.rem(z, NCLASS) < 2, value[to:to + 1], value[2 + to:3 + to])
            other = 1 - 2 * half
            for to, where in ((0, (tm, s - 1)), (0, (tm + other, s - 1)), (1, (tm + other, s))):
                pltpu.make_async_remote_copy(
                    src_ref=phold.at[to], dst_ref=prow, send_sem=psend_sem, recv_sem=precv_sem,
                    device_id=where, device_id_type=MESH).start()
            prow[...] = phold[1]

        @pl.when(jnp.logical_not(holder))
        def _():
            arrived(prow, precv_sem)

        pl.when(z < EARLY)(lambda: arrived(rows.at[pl.ds(0, 2 * NX * NY - 1)], arecv_sem))
        pl.when(z >= EARLY)(lambda: arrived(final, grecv_sem))
        sent(ysend.at[pl.ds(0, NY - 1)], ysend_sem)
        for _, _, by, _, cores in RELAYED:
            @pl.when(y == by)
            def _():
                for _ in cores:
                    sent(yvia.at[0, 0], vsend_sem)

        sent(zrecv.at[:, pl.ds(0, 4 * NZ - 4)], zsend_sem)
        pl.when((z < EARLY - 1) | last)(lambda: sent(rows, asend_sem))
        pl.when(z < EARLY)(lambda: sent(rows.at[pl.ds(0, 2 * NX * NY - 1)], asend_sem))

        @pl.when(holder)
        def _():
            for _ in range(3):
                sent(prow, psend_sem)

    ploop_out[...] = jnp.where(half == 0, prow[:, :64], prow[:, 64:])
    @pl.when(z < EARLY)
    def _():
        grand = jnp.sum(rows[...], axis=0, keepdims=True) / (NY * NCLASS * NSPACE * LANES)
        means = jnp.where(lane < 2, grand * grand, 0.0)
        final[...] = grand - jnp.where(lane == 2, jnp.sum(means, axis=1, keepdims=True), 0.0)

    for start, ends in PASS_ON:
        @pl.when((core == 1) & (z == start))
        def _():
            for end in ends:
                for to in (1, 0):
                    pltpu.make_async_remote_copy(
                        src_ref=final, dst_ref=final, send_sem=gsend_sem, recv_sem=grecv_sem,
                        device_id=(end * NY + y, x * 2 + to), device_id_type=MESH).start()
            sent(rows.at[pl.ds(0, 2 * len(ends))], gsend_sem)

    stats_out[...] = final[0, :3]


def finish(ploop_in, stats_in, ploop_out, stats_out, sems):
    copies = [pltpu.make_async_copy(ploop_in, ploop_out, sems.at[0]),
              pltpu.make_async_copy(stats_in, stats_out, sems.at[1])]
    for copy in copies:
        copy.start()
    for copy in copies:
        copy.wait()


def on_device(links):
    times_here, sites = links.shape[3:]
    rows = sites // LANES
    view = links.reshape(18, times_here, rows, LANES).transpose(0, 2, 1, 3)
    view = view.reshape(18, 8, 4, times_here, LANES)
    f32 = jnp.float32
    dma = pltpu.SemaphoreType.DMA
    vmem = pl.BlockSpec(memory_space=pltpu.VMEM)
    ploop, stats = pl.pallas_call(
        kernel,
        out_shape=(pltpu.VMEM((2, sites // 64), f32), pltpu.VMEM((3,), f32)),
        in_specs=[pl.BlockSpec(memory_space=pl.ANY)],
        out_specs=(vmem, vmem),
        scratch_shapes=[
            pltpu.VMEM((4, 4, 18, 8, LANES), f32),
            pltpu.VMEM((NY, COORDS, NCLASS, LANES), f32),
            pltpu.VMEM((2, 2, COORDS, NCLASS, LANES), f32),
            pltpu.VMEM((NY, COORDS, 2 * NCLASS, LANES), f32),
            pltpu.VMEM((NY, 18, 2 * NCLASS, LANES), f32),
            pltpu.VMEM((COORDS, 2, 4, LANES), f32),
            pltpu.VMEM((COORDS, 4 * NZ, LANES), f32),
            pltpu.VMEM((18, 4 * NZ, LANES), f32),
            pltpu.VMEM((2, 2, LANES), f32),
            pltpu.VMEM((2, LANES), f32),
            pltpu.VMEM((1, LANES), f32),
            pltpu.VMEM((2 * NX * NY, LANES), f32),
            pltpu.VMEM((1, LANES), f32),
            pltpu.SemaphoreType.REGULAR((3,)),
            dma((4,)), dma((2, 2)), dma, dma, dma((NY, 2)), dma, dma, dma, dma, dma, dma, dma, dma,
        ],
        compiler_params=pltpu.CompilerParams(collective_id=0, has_side_effects=True),
    )(view)
    hbm = pl.BlockSpec(memory_space=pl.ANY)
    return pl.pallas_call(
        finish,
        out_shape=(jax.ShapeDtypeStruct((2, sites // 64), f32), jax.ShapeDtypeStruct((3,), f32)),
        in_specs=[vmem, vmem],
        out_specs=(hbm, hbm),
        scratch_shapes=[dma((2,))],
    )(*(pltpu.with_memory_space_constraint(x, pltpu.VMEM) for x in (ploop, stats)))


def solution(mesh):
    return jax.shard_map(
        on_device, mesh=mesh, in_specs=(P(None, None, None, "tm", "space"),),
        out_specs=(P(None, ("space", "tm")), P()), check_vma=False)
```

```python
import jax
import jax.numpy as jnp
from jax import lax
from jax.experimental import pallas as pl
from jax.experimental.pallas import tpu as pltpu
from jax.sharding import PartitionSpec as P

MESH = pl.DeviceIdType.MESH
LANES = 128
NY = 8
NZ = 8
NCLASS = 4
NX = 4
NSPACE = 8
ROWS = 2
COORDS = 8
FAR_FIRST = (4, 3, 5, 2, 6, 1, 7)
Z_ORDER = (0, 7, 6, 1, 5, 2, 4, 3)
EARLY = 3
PASS_ON = ((2, (3, 4, 5, 6, 7)),)
SUM_ORDER = (0, 1, 7, 2, 6, 3, 5, 4)
RELAYED = ((0, 4, 2, 0, (1,)), (0, 4, 6, 1, (0,)), (0, 5, 6, 0, (0, 1)), (7, 4, 5, 0, (0, 1)))
PAIRS = (2, 1, 3, 0)


def third_row(a, b):
    row = []
    for i, j in ((1, 2), (2, 0), (0, 1)):
        re = (a[i][0] * b[j][0] - a[i][1] * b[j][1]) - (a[j][0] * b[i][0] - a[j][1] * b[i][1])
        im = (a[j][0] * b[i][1] + a[j][1] * b[i][0]) - (a[i][0] * b[j][1] + a[i][1] * b[j][0])
        row.append((re, im))
    return row


def product(a, b):
    return (a[0] * b[0] - a[1] * b[1], a[0] * b[1] + a[1] * b[0])


def conj_product(a, b):
    return (a[0] * b[0] + a[1] * b[1], a[0] * b[1] - a[1] * b[0])


def project(p):
    q = p[1] * p[1]
    for v in p[2:]:
        q = q + v * v
    below = p[0] < 0.0
    scale = jnp.where(below, 1.0 - p[0], 1.0) / jnp.where(below, jnp.maximum(q, 1e-20), 1.0 + p[0])
    return [jnp.where(below & (q < 1e-20), 1e-10, p[1]) * scale] + [v * scale for v in p[2:]]


def weight(x):
    n = x[0] * x[0]
    for v in x[1:]:
        n = n + v * v
    return 2.0 / (1.0 + n)


def lift(x):
    w = weight(x)
    return [w - 1.0] + [w * v for v in x]


def reflector(x):
    r = weight(x) / (1.0 + x[0] * x[0])
    return (r, r * x[0]), [(1.0, x[0]), (x[1], x[2]), (x[3], x[4])]


def coordinates(two):
    a, b = two
    x = project([v for pair in a for v in pair])
    h, u = reflector(x)
    parts = [conj_product(u[k], b[k]) for k in range(3)]
    k = conj_product(h, (parts[0][0] + parts[1][0] + parts[2][0], parts[0][1] + parts[1][1] + parts[2][1]))
    rest = []
    for j in (1, 2):
        off = product(u[j], k)
        rest += [b[j][0] - off[0], b[j][1] - off[1]]
    return x + project(rest)


def first_rows(v):
    x = v[:5]
    p = lift(x)
    q = lift(v[5:])
    h, u = reflector(x)
    one = conj_product(u[1], (q[0], q[1]))
    two = conj_product(u[2], (q[2], q[3]))
    g = product(h, (one[0] + two[0], one[1] + two[1]))
    off = [product(g, u[k]) for k in range(3)]
    return [[(p[0], p[1]), (p[2], p[3]), (p[4], p[5])],
            [(-off[0][0], -off[0][1]), (q[0] - off[1][0], q[1] - off[1][1]), (q[2] - off[2][0], q[3] - off[2][1])]]


def times(left, right):
    out = []
    for row in left:
        new = []
        for c in range(3):
            re = im = None
            for k in range(3):
                lr, li = row[k]
                rr, ri = right[k][c]
                tr = lr * rr - li * ri
                ti = lr * ri + li * rr
                re = tr if re is None else re + tr
                im = ti if im is None else im + ti
            new.append((re, im))
        out.append(new)
    return out


def full(two):
    return [two[0], two[1], third_row(two[0], two[1])]


def kernel(links, ploop_out, stats_out, lbuf, ysend, yvia, yrecv, ymat, zsend, zrecv, phold, prow, srow, rows, final,
           near_sem, load_sem, via_sem, ysend_sem, yrecv_sem, zsend_sem, zrecv_sem, precv_sem,
           asend_sem, arecv_sem, grecv_sem):
    tm = lax.axis_index("tm")
    s = lax.axis_index("space")
    z = lax.div(tm, NY)
    y = lax.rem(tm, NY)
    x = lax.div(s, 2)
    core = lax.rem(s, 2)

    def at(dz, dy, dx, to):
        return (lax.rem(z + dz + NZ, NZ) * NY + lax.rem(y + dy + NY, NY), lax.rem(x + dx, NX) * 2 + to)

    def tell(sem, whom):
        for where in whom:
            pl.semaphore_signal(sem, inc=1, device_id=where, device_id_type=MESH)

    def relayed(start, end):
        found = False
        for i, j in {(r[0], r[1]): 0 for r in RELAYED}:
            found = found | ((start == i) & (end == j))
        return found

    direct = NY - 1 - sum(jnp.where(y == i, 1, 0) for i, _ in {(r[0], r[1]): 0 for r in RELAYED})
    near = [at(1, 0, 0, 1), at(-1, 0, 0, 1), at(0, 0, 1, 1), at(0, 0, 3, 1)]
    farther = [at(2, 0, 0, 1), at(-2, 0, 0, 1), at(0, 0, 2, 1)]
    barrier = pltpu.get_barrier_semaphore()

    @pl.when(core == 1)
    def _():
        for d in FAR_FIRST:
            @pl.when(jnp.logical_not(relayed(lax.rem(y + d, NY), y)))
            def _():
                tell(barrier, [at(0, d, 0, 1), at(0, d, 0, 0)])

        tell(barrier, near + [at(0, 0, 0, 0)])

    @pl.when(core == 0)
    def _():
        tell(barrier, [at(0, 0, 0, 1)])

    pairs = PAIRS
    for k, m in enumerate(pairs):
        for t in range(4):
            pltpu.make_async_copy(links.at[:, :, m, t], lbuf.at[k, t], load_sem.at[k]).start()

    def local(k):
        pltpu.make_async_copy(lbuf.at[k], lbuf.at[k], load_sem.at[k]).wait()

        def matrix(t, rows):
            return [[(lbuf[k, t, r * 3 + c], lbuf[k, t, 9 + r * 3 + c]) for c in range(3)]
                    for r in range(rows)]

        acc = matrix(0, ROWS)
        for t in range(1, 4):
            acc = times(acc, matrix(t, 3))
        for i, v in enumerate(coordinates(acc)):
            for h in range(2):
                ysend[pairs[k] * 2 + h, i] = v[4 * h:4 * h + 4]

    def ycopy(q):
        pltpu.make_async_remote_copy(
            src_ref=ysend.at[q], dst_ref=yrecv.at[y, :, pl.ds(pl.multiple_of(core * NCLASS, NCLASS), NCLASS)],
            send_sem=ysend_sem, recv_sem=yrecv_sem.at[y], device_id=(z * NY + q, x * 2 + 1), device_id_type=MESH).start()

    for k in range(4):
        local(k)
        if k == 0:
            pl.semaphore_wait(barrier, jnp.where(core == 1, direct + len(near) + 1, direct + 1))

            @pl.when(core == 1)
            def _():
                tell(near_sem.at[0], near)

        for start, end, by, slot, cores in RELAYED:
            if k == 0:
                @pl.when((y == start) & ((core == cores[0]) | (core == cores[-1])))
                def _():
                    pltpu.make_async_remote_copy(
                        src_ref=ysend.at[end], dst_ref=yvia.at[slot, core], send_sem=ysend_sem,
                        recv_sem=via_sem.at[slot], device_id=(z * NY + by, x * 2 + 1),
                        device_id_type=MESH).start()

        for h in range(2):
            q = pairs[k] * 2 + h

            @pl.when(jnp.logical_not(relayed(y, q)) & ((q != y) | (core == 0)))
            def _():
                ycopy(q)

    def store(ref, j, mat):
        for r in range(3):
            for c in range(3):
                for p in range(2):
                    ref[j, (r * 3 + c) * 2 + p] = mat[r][c][p]

    def load(ref, j):
        return [[(ref[j, (r * 3 + c) * 2], ref[j, (r * 3 + c) * 2 + 1]) for c in range(3)] for r in range(3)]

    def sent(ref, sem):
        pltpu.make_async_remote_copy(
            src_ref=ref, dst_ref=ref, send_sem=sem, recv_sem=sem,
            device_id=at(0, 0, 0, 1 - core), device_id_type=MESH).wait_send()

    def arrived(ref, sem):
        pltpu.make_async_copy(ref, ref, sem).wait()

    half = lax.rem(y, 2)
    holder = lax.div(z, NCLASS) == half
    lane = lax.broadcasted_iota(jnp.int32, (1, LANES), 1)

    @pl.when(core == 0)
    def _():
        arrived(prow, precv_sem)
        pl.when(z < EARLY)(lambda: arrived(rows, arecv_sem))
        pl.when(z >= EARLY)(lambda: arrived(final, grecv_sem))
        sent(ysend, ysend_sem)

    @pl.when(core == 1)
    def _():
        yrecv[y, :, NCLASS:] = ysend[y]
        pl.semaphore_wait(near_sem.at[0], len(near))
        tell(near_sem.at[1], farther)

        for start, end, by, slot, cores in RELAYED:
            @pl.when(y == by)
            def _():
                arrived(yvia.at[slot] if len(cores) == 2 else yvia.at[slot, cores[0]], via_sem.at[slot])
                for to in cores:
                    pltpu.make_async_remote_copy(
                        src_ref=yvia.at[slot, to], dst_ref=yrecv.at[start, :, pl.ds(NCLASS * to, NCLASS)],
                        send_sem=ysend_sem, recv_sem=yrecv_sem.at[start], device_id=(z * NY + end, s),
                        device_id_type=MESH).start()

        for d in FAR_FIRST + (0,):
            j = lax.rem(y + d, NY)
            arrived(yrecv.at[j] if d != 0 else yrecv.at[j, :, pl.ds(0, NCLASS)], yrecv_sem.at[j])
            store(ymat, j, full(first_rows([yrecv[j, i] for i in range(COORDS)])))
        acc = load(ymat, 0)[:ROWS]
        for j in range(1, NY):
            acc = times(acc, load(ymat, j))
        for i, v in enumerate(coordinates(acc)):
            for k in range(NCLASS):
                for to in range(2):
                    row = NCLASS * to + k
                    at_row = k // 2 * 2 + to
                    zsend[i, k % 2, at_row:at_row + 1] = v[row:row + 1]

        pl.semaphore_wait(near_sem.at[1], len(farther))
        tell(near_sem.at[2], [at(0, 0, dx, 1) for dx in (2, 1, 3)] + [at(-1, 0, dx, 1) for dx in range(NX)])
        odd = lax.rem(z, 2)
        place = pl.multiple_of((odd * 4 + lax.div(z, 4) + lax.rem(lax.div(z, 2), 2) * 2) * 4, 4)
        for q in Z_ORDER:
            @pl.when(z != q)
            def _():
                pltpu.make_async_remote_copy(
                    src_ref=zsend.at[:, q % 2], dst_ref=zrecv.at[:, pl.ds(place, 4)],
                    send_sem=zsend_sem, recv_sem=zrecv_sem, device_id=(q * NY + y, s), device_id_type=MESH).start()

        zrecv[:, pl.ds(place, 4)] = zsend[:, odd]
        arrived(zrecv.at[:, pl.ds(0, 4 * NZ - 4)], zrecv_sem)

        parts = [first_rows([zrecv[i, 8 * j:8 * j + 8] for i in range(COORDS)]) for j in range(4)]
        quads = times(times(parts[0], full(parts[2])), full(times(parts[1], full(parts[3]))))
        left, right = ([[tuple(v[at_row:at_row + 4] for v in pair) for pair in row] for row in quads] for at_row in (0, 4))
        acc = times(left, full(right))
        whole = full(acc)
        re = (whole[0][0][0] + whole[1][1][0] + whole[2][2][0]) / 3.0
        im = (whole[0][0][1] + whole[1][1][1] + whole[2][2][1]) / 3.0

        def total(value):
            return jnp.sum(jnp.sum(value, axis=1, keepdims=True), axis=0, keepdims=True)

        sums = jnp.where(lane == 0, total(re), jnp.where(lane == 1, total(im), total(re * re + im * im)))
        mine = (odd * NX + x) * NY + y
        srow[...] = sums
        pl.semaphore_wait(near_sem.at[2], 2 * NX - 1)
        last = z == NZ - 1
        for step in (0, 1):
            dz = jnp.where(last, 1 - step, step)
            end = lax.rem(z + dz, NZ)

            @pl.when(end < EARLY)
            def _():
                for to in (1, 0):
                    for q in SUM_ORDER:
                        for to_x in (0, 1, 3, 2):
                            def send():
                                pltpu.make_async_remote_copy(
                                    src_ref=srow, dst_ref=rows.at[pl.ds(mine, 1)], send_sem=asend_sem, recv_sem=arecv_sem,
                                    device_id=(end * NY + q, to_x * 2 + to), device_id_type=MESH).start()

                            if to == 1:
                                pl.when((dz != 0) | (y != q) | (x != to_x))(send)
                            else:
                                send()

        rows[pl.ds(mine, 1)] = sums
        @pl.when(holder)
        def _():
            for to in range(2):
                for p, value in enumerate((re, im)):
                    phold[to, p:p + 1] = jnp.where(lax.rem(z, NCLASS) < 2, value[to:to + 1], value[2 + to:3 + to])
            other = 1 - 2 * half
            for to, where in ((0, (tm, s - 1)), (0, (tm + other, s - 1)), (1, (tm + other, s))):
                pltpu.make_async_remote_copy(
                    src_ref=phold.at[to], dst_ref=prow, send_sem=asend_sem, recv_sem=precv_sem,
                    device_id=where, device_id_type=MESH).start()
            prow[...] = phold[1]

        @pl.when(jnp.logical_not(holder))
        def _():
            arrived(prow, precv_sem)

        pl.when(z < EARLY)(lambda: arrived(rows.at[pl.ds(0, 2 * NX * NY - 1)], arecv_sem))
        pl.when(z >= EARLY)(lambda: arrived(final, grecv_sem))
        sent(ysend.at[pl.ds(0, NY - 1)], ysend_sem)
        for _, _, by, _, cores in RELAYED:
            @pl.when(y == by)
            def _():
                for _ in cores:
                    sent(yvia.at[0, 0], ysend_sem)

        sent(zrecv.at[:, pl.ds(0, 4 * NZ - 4)], zsend_sem)
        pl.when((z < EARLY - 1) | last)(lambda: sent(rows, asend_sem))
        pl.when(z < EARLY)(lambda: sent(rows.at[pl.ds(0, 2 * NX * NY - 1)], asend_sem))

        @pl.when(holder)
        def _():
            for _ in range(3):
                sent(prow, asend_sem)

    ploop_out[...] = jnp.where(half == 0, prow[:, :64], prow[:, 64:])
    @pl.when(z < EARLY)
    def _():
        grand = jnp.sum(rows[...], axis=0, keepdims=True) / (NY * NCLASS * NSPACE * LANES)
        means = jnp.where(lane < 2, grand * grand, 0.0)
        final[...] = grand - jnp.where(lane == 2, jnp.sum(means, axis=1, keepdims=True), 0.0)

    for start, ends in PASS_ON:
        @pl.when((core == 1) & (z == start))
        def _():
            for end in ends:
                for to in (1, 0):
                    pltpu.make_async_remote_copy(
                        src_ref=final, dst_ref=final, send_sem=asend_sem, recv_sem=grecv_sem,
                        device_id=(end * NY + y, x * 2 + to), device_id_type=MESH).start()
            sent(rows.at[pl.ds(0, 2 * len(ends))], asend_sem)

    stats_out[...] = final[0, :3]


def finish(ploop_in, stats_in, ploop_out, stats_out, sems):
    copies = [pltpu.make_async_copy(ploop_in, ploop_out, sems.at[0]),
              pltpu.make_async_copy(stats_in, stats_out, sems.at[1])]
    for copy in copies:
        copy.start()
    for copy in copies:
        copy.wait()


def on_device(links):
    times_here, sites = links.shape[3:]
    rows = sites // LANES
    view = links.reshape(18, times_here, rows, LANES).transpose(0, 2, 1, 3)
    view = view.reshape(18, 8, 4, times_here, LANES)
    f32 = jnp.float32
    dma = pltpu.SemaphoreType.DMA
    vmem = pl.BlockSpec(memory_space=pltpu.VMEM)
    ploop, stats = pl.pallas_call(
        kernel,
        out_shape=(pltpu.VMEM((2, sites // 64), f32), pltpu.VMEM((3,), f32)),
        in_specs=[pl.BlockSpec(memory_space=pl.ANY)],
        out_specs=(vmem, vmem),
        scratch_shapes=[
            pltpu.VMEM((4, 4, 18, 8, LANES), f32),
            pltpu.VMEM((NY, COORDS, NCLASS, LANES), f32),
            pltpu.VMEM((2, 2, COORDS, NCLASS, LANES), f32),
            pltpu.VMEM((NY, COORDS, 2 * NCLASS, LANES), f32),
            pltpu.VMEM((NY, 18, 2 * NCLASS, LANES), f32),
            pltpu.VMEM((COORDS, 2, 4, LANES), f32),
            pltpu.VMEM((COORDS, 4 * NZ, LANES), f32),
            pltpu.VMEM((2, 2, LANES), f32),
            pltpu.VMEM((2, LANES), f32),
            pltpu.VMEM((1, LANES), f32),
            pltpu.VMEM((2 * NX * NY, LANES), f32),
            pltpu.VMEM((1, LANES), f32),
            pltpu.SemaphoreType.REGULAR((3,)),
            dma((4,)), dma((2,)), dma, dma((NY,)), dma, dma, dma, dma, dma, dma,
        ],
        compiler_params=pltpu.CompilerParams(collective_id=0, has_side_effects=True),
    )(view)
    hbm = pl.BlockSpec(memory_space=pl.ANY)
    return pl.pallas_call(
        finish,
        out_shape=(jax.ShapeDtypeStruct((2, sites // 64), f32), jax.ShapeDtypeStruct((3,), f32)),
        in_specs=[vmem, vmem],
        out_specs=(hbm, hbm),
        scratch_shapes=[dma((2,))],
    )(*(pltpu.with_memory_space_constraint(x, pltpu.VMEM) for x in (ploop, stats)))


def solution(mesh):
    return jax.shard_map(
        on_device, mesh=mesh, in_specs=(P(None, None, None, "tm", "space"),),
        out_specs=(P(None, ("space", "tm")), P()), check_vma=False)
```

```python
import jax
import jax.numpy as jnp
from jax import lax
from jax.experimental import pallas as pl
from jax.experimental.pallas import tpu as pltpu
from jax.sharding import PartitionSpec as P

MESH = pl.DeviceIdType.MESH
LANES = 128
NY = 8
NZ = 8
NCLASS = 4
NX = 4
NSPACE = 8
ROWS = 2
COORDS = 8
FAR_FIRST = (4, 3, 5, 2, 6, 1, 7)
Z_ORDER = (0, 7, 6, 1, 5, 2, 4, 3)
EARLY = 3
PASS_ON = ((2, (3, 4, 5, 6, 7)),)
SUM_ORDER = (0, 1, 7, 2, 6, 3, 5, 4)
RELAYED = ((0, 4, 2, 0, (1,)), (0, 4, 6, 1, (0,)), (0, 5, 6, 0, (0, 1)), (7, 4, 5, 0, (0, 1)))
PAIRS = (2, 1, 3, 0)
PAIRS_0 = (2, 3, 1, 0)


def third_row(a, b):
    row = []
    for i, j in ((1, 2), (2, 0), (0, 1)):
        re = (a[i][0] * b[j][0] - a[i][1] * b[j][1]) - (a[j][0] * b[i][0] - a[j][1] * b[i][1])
        im = (a[j][0] * b[i][1] + a[j][1] * b[i][0]) - (a[i][0] * b[j][1] + a[i][1] * b[j][0])
        row.append((re, im))
    return row


def product(a, b):
    return (a[0] * b[0] - a[1] * b[1], a[0] * b[1] + a[1] * b[0])


def conj_product(a, b):
    return (a[0] * b[0] + a[1] * b[1], a[0] * b[1] - a[1] * b[0])


def project(p):
    q = p[1] * p[1]
    for v in p[2:]:
        q = q + v * v
    below = p[0] < 0.0
    scale = jnp.where(below, 1.0 - p[0], 1.0) / jnp.where(below, jnp.maximum(q, 1e-20), 1.0 + p[0])
    return [jnp.where(below & (q < 1e-20), 1e-10, p[1]) * scale] + [v * scale for v in p[2:]]


def weight(x):
    n = x[0] * x[0]
    for v in x[1:]:
        n = n + v * v
    return 2.0 / (1.0 + n)


def lift(x):
    w = weight(x)
    return [w - 1.0] + [w * v for v in x]


def reflector(x):
    r = weight(x) / (1.0 + x[0] * x[0])
    return (r, r * x[0]), [(1.0, x[0]), (x[1], x[2]), (x[3], x[4])]


def coordinates(two):
    a, b = two
    x = project([v for pair in a for v in pair])
    h, u = reflector(x)
    parts = [conj_product(u[k], b[k]) for k in range(3)]
    k = conj_product(h, (parts[0][0] + parts[1][0] + parts[2][0], parts[0][1] + parts[1][1] + parts[2][1]))
    rest = []
    for j in (1, 2):
        off = product(u[j], k)
        rest += [b[j][0] - off[0], b[j][1] - off[1]]
    return x + project(rest)


def first_rows(v):
    x = v[:5]
    p = lift(x)
    q = lift(v[5:])
    h, u = reflector(x)
    one = conj_product(u[1], (q[0], q[1]))
    two = conj_product(u[2], (q[2], q[3]))
    g = product(h, (one[0] + two[0], one[1] + two[1]))
    off = [product(g, u[k]) for k in range(3)]
    return [[(p[0], p[1]), (p[2], p[3]), (p[4], p[5])],
            [(-off[0][0], -off[0][1]), (q[0] - off[1][0], q[1] - off[1][1]), (q[2] - off[2][0], q[3] - off[2][1])]]


def times(left, right):
    out = []
    for row in left:
        new = []
        for c in range(3):
            re = im = None
            for k in range(3):
                lr, li = row[k]
                rr, ri = right[k][c]
                tr = lr * rr - li * ri
                ti = lr * ri + li * rr
                re = tr if re is None else re + tr
                im = ti if im is None else im + ti
            new.append((re, im))
        out.append(new)
    return out


def full(two):
    return [two[0], two[1], third_row(two[0], two[1])]


def kernel(links, ploop_out, stats_out, lbuf, ysend, yvia, yrecv, ymat, zsend, zrecv, phold, prow, srow, rows, final,
           near_sem, load_sem, via_sem, ysend_sem, yrecv_sem, zsend_sem, zrecv_sem, precv_sem,
           asend_sem, arecv_sem, grecv_sem):
    tm = lax.axis_index("tm")
    s = lax.axis_index("space")
    z = lax.div(tm, NY)
    y = lax.rem(tm, NY)
    x = lax.div(s, 2)
    core = lax.rem(s, 2)

    def at(dz, dy, dx, to):
        return (lax.rem(z + dz + NZ, NZ) * NY + lax.rem(y + dy + NY, NY), lax.rem(x + dx, NX) * 2 + to)

    def tell(sem, whom):
        for where in whom:
            pl.semaphore_signal(sem, inc=1, device_id=where, device_id_type=MESH)

    def relayed(start, end):
        found = False
        for i, j in {(r[0], r[1]): 0 for r in RELAYED}:
            found = found | ((start == i) & (end == j))
        return found

    direct = NY - 1 - sum(jnp.where(y == i, 1, 0) for i, _ in {(r[0], r[1]): 0 for r in RELAYED})
    near = [at(1, 0, 0, 1), at(-1, 0, 0, 1), at(0, 0, 1, 1), at(0, 0, 3, 1)]
    farther = [at(2, 0, 0, 1), at(-2, 0, 0, 1), at(0, 0, 2, 1)]
    barrier = pltpu.get_barrier_semaphore()

    @pl.when(core == 1)
    def _():
        for d in FAR_FIRST:
            @pl.when(jnp.logical_not(relayed(lax.rem(y + d, NY), y)))
            def _():
                tell(barrier, [at(0, d, 0, 1), at(0, d, 0, 0)])

        tell(barrier, near + [at(0, 0, 0, 0)])

    @pl.when(core == 0)
    def _():
        tell(barrier, [at(0, 0, 0, 1)])

    pairs = [jnp.where(core == 1, m, n) for m, n in zip(PAIRS, PAIRS_0)]
    for k, m in enumerate(pairs):
        for t in range(4):
            pltpu.make_async_copy(links.at[:, :, m, t], lbuf.at[k, t], load_sem.at[k]).start()

    def local(k):
        pltpu.make_async_copy(lbuf.at[k], lbuf.at[k], load_sem.at[k]).wait()

        def matrix(t, rows):
            return [[(lbuf[k, t, r * 3 + c], lbuf[k, t, 9 + r * 3 + c]) for c in range(3)]
                    for r in range(rows)]

        acc = matrix(0, ROWS)
        for t in range(1, 4):
            acc = times(acc, matrix(t, 3))
        for i, v in enumerate(coordinates(acc)):
            for h in range(2):
                ysend[pairs[k] * 2 + h, i] = v[4 * h:4 * h + 4]

    def ycopy(q):
        pltpu.make_async_remote_copy(
            src_ref=ysend.at[q], dst_ref=yrecv.at[y, :, pl.ds(pl.multiple_of(core * NCLASS, NCLASS), NCLASS)],
            send_sem=ysend_sem, recv_sem=yrecv_sem.at[y], device_id=(z * NY + q, x * 2 + 1), device_id_type=MESH).start()

    for k in range(4):
        local(k)
        if k == 0:
            pl.semaphore_wait(barrier, jnp.where(core == 1, direct + len(near) + 1, direct + 1))

            @pl.when(core == 1)
            def _():
                tell(near_sem.at[0], near)

        for start, end, by, slot, cores in RELAYED:
            if k == 0:
                @pl.when((y == start) & ((core == cores[0]) | (core == cores[-1])))
                def _():
                    pltpu.make_async_remote_copy(
                        src_ref=ysend.at[end], dst_ref=yvia.at[slot, core], send_sem=ysend_sem,
                        recv_sem=via_sem.at[slot], device_id=(z * NY + by, x * 2 + 1),
                        device_id_type=MESH).start()

        for h in range(2):
            q = pairs[k] * 2 + h

            @pl.when(jnp.logical_not(relayed(y, q)) & ((q != y) | (core == 0)))
            def _():
                ycopy(q)

    def store(ref, j, mat):
        for r in range(3):
            for c in range(3):
                for p in range(2):
                    ref[j, (r * 3 + c) * 2 + p] = mat[r][c][p]

    def load(ref, j):
        return [[(ref[j, (r * 3 + c) * 2], ref[j, (r * 3 + c) * 2 + 1]) for c in range(3)] for r in range(3)]

    def sent(ref, sem):
        pltpu.make_async_remote_copy(
            src_ref=ref, dst_ref=ref, send_sem=sem, recv_sem=sem,
            device_id=at(0, 0, 0, 1 - core), device_id_type=MESH).wait_send()

    def arrived(ref, sem):
        pltpu.make_async_copy(ref, ref, sem).wait()

    half = lax.rem(y, 2)
    holder = lax.div(z, NCLASS) == half
    lane = lax.broadcasted_iota(jnp.int32, (1, LANES), 1)

    @pl.when(core == 0)
    def _():
        arrived(prow, precv_sem)
        pl.when(z < EARLY)(lambda: arrived(rows, arecv_sem))
        pl.when(z >= EARLY)(lambda: arrived(final, grecv_sem))
        sent(ysend, ysend_sem)

    @pl.when(core == 1)
    def _():
        yrecv[y, :, NCLASS:] = ysend[y]
        pl.semaphore_wait(near_sem.at[0], len(near))
        tell(near_sem.at[1], farther)

        for start, end, by, slot, cores in RELAYED:
            @pl.when(y == by)
            def _():
                arrived(yvia.at[slot] if len(cores) == 2 else yvia.at[slot, cores[0]], via_sem.at[slot])
                for to in cores:
                    pltpu.make_async_remote_copy(
                        src_ref=yvia.at[slot, to], dst_ref=yrecv.at[start, :, pl.ds(NCLASS * to, NCLASS)],
                        send_sem=ysend_sem, recv_sem=yrecv_sem.at[start], device_id=(z * NY + end, s),
                        device_id_type=MESH).start()

        for d in FAR_FIRST + (0,):
            j = lax.rem(y + d, NY)
            arrived(yrecv.at[j] if d != 0 else yrecv.at[j, :, pl.ds(0, NCLASS)], yrecv_sem.at[j])
            store(ymat, j, full(first_rows([yrecv[j, i] for i in range(COORDS)])))
        acc = load(ymat, 0)[:ROWS]
        for j in range(1, NY):
            acc = times(acc, load(ymat, j))
        for i, v in enumerate(coordinates(acc)):
            for k in range(NCLASS):
                for to in range(2):
                    row = NCLASS * to + k
                    at_row = k // 2 * 2 + to
                    zsend[i, k % 2, at_row:at_row + 1] = v[row:row + 1]

        pl.semaphore_wait(near_sem.at[1], len(farther))
        tell(near_sem.at[2], [at(0, 0, dx, 1) for dx in (2, 1, 3)] + [at(-1, 0, dx, 1) for dx in range(NX)])
        odd = lax.rem(z, 2)
        place = pl.multiple_of((odd * 4 + lax.div(z, 4) + lax.rem(lax.div(z, 2), 2) * 2) * 4, 4)
        for q in Z_ORDER:
            @pl.when(z != q)
            def _():
                pltpu.make_async_remote_copy(
                    src_ref=zsend.at[:, q % 2], dst_ref=zrecv.at[:, pl.ds(place, 4)],
                    send_sem=zsend_sem, recv_sem=zrecv_sem, device_id=(q * NY + y, s), device_id_type=MESH).start()

        zrecv[:, pl.ds(place, 4)] = zsend[:, odd]
        arrived(zrecv.at[:, pl.ds(0, 4 * NZ - 4)], zrecv_sem)

        parts = [first_rows([zrecv[i, 8 * j:8 * j + 8] for i in range(COORDS)]) for j in range(4)]
        quads = times(times(parts[0], full(parts[2])), full(times(parts[1], full(parts[3]))))
        left, right = ([[tuple(v[at_row:at_row + 4] for v in pair) for pair in row] for row in quads] for at_row in (0, 4))
        acc = times(left, full(right))
        whole = full(acc)
        re = (whole[0][0][0] + whole[1][1][0] + whole[2][2][0]) / 3.0
        im = (whole[0][0][1] + whole[1][1][1] + whole[2][2][1]) / 3.0

        def total(value):
            return jnp.sum(jnp.sum(value, axis=1, keepdims=True), axis=0, keepdims=True)

        sums = jnp.where(lane == 0, total(re), jnp.where(lane == 1, total(im), total(re * re + im * im)))
        mine = (odd * NX + x) * NY + y
        srow[...] = sums
        pl.semaphore_wait(near_sem.at[2], 2 * NX - 1)
        last = z == NZ - 1
        for step in (0, 1):
            dz = jnp.where(last, 1 - step, step)
            end = lax.rem(z + dz, NZ)

            @pl.when(end < EARLY)
            def _():
                for to in (1, 0):
                    for q in SUM_ORDER:
                        for to_x in (0, 1, 3, 2):
                            def send():
                                pltpu.make_async_remote_copy(
                                    src_ref=srow, dst_ref=rows.at[pl.ds(mine, 1)], send_sem=asend_sem, recv_sem=arecv_sem,
                                    device_id=(end * NY + q, to_x * 2 + to), device_id_type=MESH).start()

                            if to == 1:
                                pl.when((dz != 0) | (y != q) | (x != to_x))(send)
                            else:
                                send()

        rows[pl.ds(mine, 1)] = sums
        @pl.when(holder)
        def _():
            for to in range(2):
                for p, value in enumerate((re, im)):
                    phold[to, p:p + 1] = jnp.where(lax.rem(z, NCLASS) < 2, value[to:to + 1], value[2 + to:3 + to])
            other = 1 - 2 * half
            for to, where in ((0, (tm, s - 1)), (0, (tm + other, s - 1)), (1, (tm + other, s))):
                pltpu.make_async_remote_copy(
                    src_ref=phold.at[to], dst_ref=prow, send_sem=asend_sem, recv_sem=precv_sem,
                    device_id=where, device_id_type=MESH).start()
            prow[...] = phold[1]

        @pl.when(jnp.logical_not(holder))
        def _():
            arrived(prow, precv_sem)

        pl.when(z < EARLY)(lambda: arrived(rows.at[pl.ds(0, 2 * NX * NY - 1)], arecv_sem))
        pl.when(z >= EARLY)(lambda: arrived(final, grecv_sem))
        sent(ysend.at[pl.ds(0, NY - 1)], ysend_sem)
        for _, _, by, _, cores in RELAYED:
            @pl.when(y == by)
            def _():
                for _ in cores:
                    sent(yvia.at[0, 0], ysend_sem)

        sent(zrecv.at[:, pl.ds(0, 4 * NZ - 4)], zsend_sem)
        pl.when((z < EARLY - 1) | last)(lambda: sent(rows, asend_sem))
        pl.when(z < EARLY)(lambda: sent(rows.at[pl.ds(0, 2 * NX * NY - 1)], asend_sem))

        @pl.when(holder)
        def _():
            for _ in range(3):
                sent(prow, asend_sem)

    ploop_out[...] = jnp.where(half == 0, prow[:, :64], prow[:, 64:])
    @pl.when(z < EARLY)
    def _():
        grand = jnp.sum(rows[...], axis=0, keepdims=True) / (NY * NCLASS * NSPACE * LANES)
        means = jnp.where(lane < 2, grand * grand, 0.0)
        final[...] = grand - jnp.where(lane == 2, jnp.sum(means, axis=1, keepdims=True), 0.0)

    for start, ends in PASS_ON:
        @pl.when((core == 1) & (z == start))
        def _():
            for end in ends:
                for to in (1, 0):
                    pltpu.make_async_remote_copy(
                        src_ref=final, dst_ref=final, send_sem=asend_sem, recv_sem=grecv_sem,
                        device_id=(end * NY + y, x * 2 + to), device_id_type=MESH).start()
            sent(rows.at[pl.ds(0, 2 * len(ends))], asend_sem)

    stats_out[...] = final[0, :3]


def finish(ploop_in, stats_in, ploop_out, stats_out, sems):
    copies = [pltpu.make_async_copy(ploop_in, ploop_out, sems.at[0]),
              pltpu.make_async_copy(stats_in, stats_out, sems.at[1])]
    for copy in copies:
        copy.start()
    for copy in copies:
        copy.wait()


def on_device(links):
    times_here, sites = links.shape[3:]
    rows = sites // LANES
    view = links.reshape(18, times_here, rows, LANES).transpose(0, 2, 1, 3)
    view = view.reshape(18, 8, 4, times_here, LANES)
    f32 = jnp.float32
    dma = pltpu.SemaphoreType.DMA
    vmem = pl.BlockSpec(memory_space=pltpu.VMEM)
    ploop, stats = pl.pallas_call(
        kernel,
        out_shape=(pltpu.VMEM((2, sites // 64), f32), pltpu.VMEM((3,), f32)),
        in_specs=[pl.BlockSpec(memory_space=pl.ANY)],
        out_specs=(vmem, vmem),
        scratch_shapes=[
            pltpu.VMEM((4, 4, 18, 8, LANES), f32),
            pltpu.VMEM((NY, COORDS, NCLASS, LANES), f32),
            pltpu.VMEM((2, 2, COORDS, NCLASS, LANES), f32),
            pltpu.VMEM((NY, COORDS, 2 * NCLASS, LANES), f32),
            pltpu.VMEM((NY, 18, 2 * NCLASS, LANES), f32),
            pltpu.VMEM((COORDS, 2, 4, LANES), f32),
            pltpu.VMEM((COORDS, 4 * NZ, LANES), f32),
            pltpu.VMEM((2, 2, LANES), f32),
            pltpu.VMEM((2, LANES), f32),
            pltpu.VMEM((1, LANES), f32),
            pltpu.VMEM((2 * NX * NY, LANES), f32),
            pltpu.VMEM((1, LANES), f32),
            pltpu.SemaphoreType.REGULAR((3,)),
            dma((4,)), dma((2,)), dma, dma((NY,)), dma, dma, dma, dma, dma, dma,
        ],
        compiler_params=pltpu.CompilerParams(collective_id=0, has_side_effects=True),
    )(view)
    hbm = pl.BlockSpec(memory_space=pl.ANY)
    return pl.pallas_call(
        finish,
        out_shape=(jax.ShapeDtypeStruct((2, sites // 64), f32), jax.ShapeDtypeStruct((3,), f32)),
        in_specs=[vmem, vmem],
        out_specs=(hbm, hbm),
        scratch_shapes=[dma((2,))],
    )(*(pltpu.with_memory_space_constraint(x, pltpu.VMEM) for x in (ploop, stats)))


def solution(mesh):
    return jax.shard_map(
        on_device, mesh=mesh, in_specs=(P(None, None, None, "tm", "space"),),
        out_specs=(P(None, ("space", "tm")), P()), check_vma=False)
```

```python
import jax
import jax.numpy as jnp
from jax import lax
from jax.experimental import pallas as pl
from jax.experimental.pallas import tpu as pltpu
from jax.sharding import PartitionSpec as P

MESH = pl.DeviceIdType.MESH
LANES = 128
NY = 8
NZ = 8
NCLASS = 4
NX = 4
NSPACE = 8
ROWS = 2
COORDS = 8
FAR_FIRST = (4, 3, 5, 2, 6, 1, 7)
Z_ORDER = (0, 7, 1, 2, 6, 5, 4, 3)
EARLY = 3
PASS_ON = ((2, (3, 4, 5, 6, 7)),)
SUM_ORDER = (0, 1, 7, 2, 6, 3, 5, 4)
RELAYED = ((0, 4, 2, 0, (1,)), (0, 4, 6, 1, (0,)), (0, 5, 6, 0, (0, 1)), (7, 4, 5, 0, (0, 1)))
PAIRS = (2, 1, 3, 0)
PAIRS_0 = (2, 3, 1, 0)


def third_row(a, b):
    row = []
    for i, j in ((1, 2), (2, 0), (0, 1)):
        re = (a[i][0] * b[j][0] - a[i][1] * b[j][1]) - (a[j][0] * b[i][0] - a[j][1] * b[i][1])
        im = (a[j][0] * b[i][1] + a[j][1] * b[i][0]) - (a[i][0] * b[j][1] + a[i][1] * b[j][0])
        row.append((re, im))
    return row


def product(a, b):
    return (a[0] * b[0] - a[1] * b[1], a[0] * b[1] + a[1] * b[0])


def conj_product(a, b):
    return (a[0] * b[0] + a[1] * b[1], a[0] * b[1] - a[1] * b[0])


def project(p):
    q = p[1] * p[1]
    for v in p[2:]:
        q = q + v * v
    below = p[0] < 0.0
    scale = jnp.where(below, 1.0 - p[0], 1.0) / jnp.where(below, jnp.maximum(q, 1e-20), 1.0 + p[0])
    return [jnp.where(below & (q < 1e-20), 1e-10, p[1]) * scale] + [v * scale for v in p[2:]]


def weight(x):
    n = x[0] * x[0]
    for v in x[1:]:
        n = n + v * v
    return 2.0 / (1.0 + n)


def lift(x):
    w = weight(x)
    return [w - 1.0] + [w * v for v in x]


def reflector(x):
    r = weight(x) / (1.0 + x[0] * x[0])
    return (r, r * x[0]), [(1.0, x[0]), (x[1], x[2]), (x[3], x[4])]


def coordinates(two):
    a, b = two
    x = project([v for pair in a for v in pair])
    h, u = reflector(x)
    parts = [conj_product(u[k], b[k]) for k in range(3)]
    k = conj_product(h, (parts[0][0] + parts[1][0] + parts[2][0], parts[0][1] + parts[1][1] + parts[2][1]))
    rest = []
    for j in (1, 2):
        off = product(u[j], k)
        rest += [b[j][0] - off[0], b[j][1] - off[1]]
    return x + project(rest)


def first_rows(v):
    x = v[:5]
    p = lift(x)
    q = lift(v[5:])
    h, u = reflector(x)
    one = conj_product(u[1], (q[0], q[1]))
    two = conj_product(u[2], (q[2], q[3]))
    g = product(h, (one[0] + two[0], one[1] + two[1]))
    off = [product(g, u[k]) for k in range(3)]
    return [[(p[0], p[1]), (p[2], p[3]), (p[4], p[5])],
            [(-off[0][0], -off[0][1]), (q[0] - off[1][0], q[1] - off[1][1]), (q[2] - off[2][0], q[3] - off[2][1])]]


def times(left, right):
    out = []
    for row in left:
        new = []
        for c in range(3):
            re = im = None
            for k in range(3):
                lr, li = row[k]
                rr, ri = right[k][c]
                tr = lr * rr - li * ri
                ti = lr * ri + li * rr
                re = tr if re is None else re + tr
                im = ti if im is None else im + ti
            new.append((re, im))
        out.append(new)
    return out


def full(two):
    return [two[0], two[1], third_row(two[0], two[1])]


def kernel(links, ploop_out, stats_out, lbuf, ysend, yvia, yrecv, ymat, zsend, zrecv, phold, prow, srow, rows, final,
           near_sem, load_sem, via_sem, ysend_sem, yrecv_sem, zsend_sem, zrecv_sem, precv_sem,
           asend_sem, arecv_sem, grecv_sem):
    tm = lax.axis_index("tm")
    s = lax.axis_index("space")
    z = lax.div(tm, NY)
    y = lax.rem(tm, NY)
    x = lax.div(s, 2)
    core = lax.rem(s, 2)

    def at(dz, dy, dx, to):
        return (lax.rem(z + dz + NZ, NZ) * NY + lax.rem(y + dy + NY, NY), lax.rem(x + dx, NX) * 2 + to)

    def tell(sem, whom):
        for where in whom:
            pl.semaphore_signal(sem, inc=1, device_id=where, device_id_type=MESH)

    def relayed(start, end):
        found = False
        for i, j in {(r[0], r[1]): 0 for r in RELAYED}:
            found = found | ((start == i) & (end == j))
        return found

    direct = NY - 1 - sum(jnp.where(y == i, 1, 0) for i, _ in {(r[0], r[1]): 0 for r in RELAYED})
    near = [at(1, 0, 0, 1), at(-1, 0, 0, 1), at(0, 0, 1, 1), at(0, 0, 3, 1)]
    farther = [at(2, 0, 0, 1), at(-2, 0, 0, 1), at(0, 0, 2, 1)]
    barrier = pltpu.get_barrier_semaphore()

    @pl.when(core == 1)
    def _():
        for d in FAR_FIRST:
            @pl.when(jnp.logical_not(relayed(lax.rem(y + d, NY), y)))
            def _():
                tell(barrier, [at(0, d, 0, 1), at(0, d, 0, 0)])

        tell(barrier, near + [at(0, 0, 0, 0)])

    @pl.when(core == 0)
    def _():
        tell(barrier, [at(0, 0, 0, 1)])

    pairs = [jnp.where(core == 1, m, n) for m, n in zip(PAIRS, PAIRS_0)]
    for k, m in enumerate(pairs):
        for t in range(4):
            pltpu.make_async_copy(links.at[:, :, m, t], lbuf.at[k, t], load_sem.at[k]).start()

    def local(k):
        pltpu.make_async_copy(lbuf.at[k], lbuf.at[k], load_sem.at[k]).wait()

        def matrix(t, rows):
            return [[(lbuf[k, t, r * 3 + c], lbuf[k, t, 9 + r * 3 + c]) for c in range(3)]
                    for r in range(rows)]

        acc = matrix(0, ROWS)
        for t in range(1, 4):
            acc = times(acc, matrix(t, 3))
        for i, v in enumerate(coordinates(acc)):
            for h in range(2):
                ysend[pairs[k] * 2 + h, i] = v[4 * h:4 * h + 4]

    def ycopy(q):
        pltpu.make_async_remote_copy(
            src_ref=ysend.at[q], dst_ref=yrecv.at[y, :, pl.ds(pl.multiple_of(core * NCLASS, NCLASS), NCLASS)],
            send_sem=ysend_sem, recv_sem=yrecv_sem.at[y], device_id=(z * NY + q, x * 2 + 1), device_id_type=MESH).start()

    for k in range(4):
        local(k)
        if k == 0:
            pl.semaphore_wait(barrier, jnp.where(core == 1, direct + len(near) + 1, direct + 1))

            @pl.when(core == 1)
            def _():
                tell(near_sem.at[0], near)

        for start, end, by, slot, cores in RELAYED:
            if k == 0:
                @pl.when((y == start) & ((core == cores[0]) | (core == cores[-1])))
                def _():
                    pltpu.make_async_remote_copy(
                        src_ref=ysend.at[end], dst_ref=yvia.at[slot, core], send_sem=ysend_sem,
                        recv_sem=via_sem.at[slot], device_id=(z * NY + by, x * 2 + 1),
                        device_id_type=MESH).start()

        for h in range(2):
            q = pairs[k] * 2 + h

            @pl.when(jnp.logical_not(relayed(y, q)) & ((q != y) | (core == 0)))
            def _():
                ycopy(q)

    def store(ref, j, mat):
        for r in range(3):
            for c in range(3):
                for p in range(2):
                    ref[j, (r * 3 + c) * 2 + p] = mat[r][c][p]

    def load(ref, j):
        return [[(ref[j, (r * 3 + c) * 2], ref[j, (r * 3 + c) * 2 + 1]) for c in range(3)] for r in range(3)]

    def sent(ref, sem):
        pltpu.make_async_remote_copy(
            src_ref=ref, dst_ref=ref, send_sem=sem, recv_sem=sem,
            device_id=at(0, 0, 0, 1 - core), device_id_type=MESH).wait_send()

    def arrived(ref, sem):
        pltpu.make_async_copy(ref, ref, sem).wait()

    half = lax.rem(y, 2)
    holder = lax.div(z, NCLASS) == half
    lane = lax.broadcasted_iota(jnp.int32, (1, LANES), 1)

    @pl.when(core == 0)
    def _():
        arrived(prow, precv_sem)
        pl.when(z < EARLY)(lambda: arrived(rows, arecv_sem))
        pl.when(z >= EARLY)(lambda: arrived(final, grecv_sem))
        sent(ysend, ysend_sem)

    @pl.when(core == 1)
    def _():
        yrecv[y, :, NCLASS:] = ysend[y]
        pl.semaphore_wait(near_sem.at[0], len(near))
        tell(near_sem.at[1], farther)

        for start, end, by, slot, cores in RELAYED:
            @pl.when(y == by)
            def _():
                arrived(yvia.at[slot] if len(cores) == 2 else yvia.at[slot, cores[0]], via_sem.at[slot])
                for to in cores:
                    pltpu.make_async_remote_copy(
                        src_ref=yvia.at[slot, to], dst_ref=yrecv.at[start, :, pl.ds(NCLASS * to, NCLASS)],
                        send_sem=ysend_sem, recv_sem=yrecv_sem.at[start], device_id=(z * NY + end, s),
                        device_id_type=MESH).start()

        for d in FAR_FIRST + (0,):
            j = lax.rem(y + d, NY)
            arrived(yrecv.at[j] if d != 0 else yrecv.at[j, :, pl.ds(0, NCLASS)], yrecv_sem.at[j])
            store(ymat, j, full(first_rows([yrecv[j, i] for i in range(COORDS)])))
        acc = load(ymat, 0)[:ROWS]
        for j in range(1, NY):
            acc = times(acc, load(ymat, j))
        for i, v in enumerate(coordinates(acc)):
            for k in range(NCLASS):
                for to in range(2):
                    row = NCLASS * to + k
                    at_row = k // 2 * 2 + to
                    zsend[i, k % 2, at_row:at_row + 1] = v[row:row + 1]

        pl.semaphore_wait(near_sem.at[1], len(farther))
        tell(near_sem.at[2], [at(0, 0, dx, 1) for dx in (2, 1, 3)] + [at(-1, 0, dx, 1) for dx in range(NX)])
        odd = lax.rem(z, 2)
        place = pl.multiple_of((odd * 4 + lax.div(z, 4) + lax.rem(lax.div(z, 2), 2) * 2) * 4, 4)
        for q in Z_ORDER:
            @pl.when(z != q)
            def _():
                pltpu.make_async_remote_copy(
                    src_ref=zsend.at[:, q % 2], dst_ref=zrecv.at[:, pl.ds(place, 4)],
                    send_sem=zsend_sem, recv_sem=zrecv_sem, device_id=(q * NY + y, s), device_id_type=MESH).start()

        zrecv[:, pl.ds(place, 4)] = zsend[:, odd]
        arrived(zrecv.at[:, pl.ds(0, 4 * NZ - 4)], zrecv_sem)

        parts = [first_rows([zrecv[i, 8 * j:8 * j + 8] for i in range(COORDS)]) for j in range(4)]
        quads = times(times(parts[0], full(parts[2])), full(times(parts[1], full(parts[3]))))
        left, right = ([[tuple(v[at_row:at_row + 4] for v in pair) for pair in row] for row in quads] for at_row in (0, 4))
        acc = times(left, full(right))
        whole = full(acc)
        re = (whole[0][0][0] + whole[1][1][0] + whole[2][2][0]) / 3.0
        im = (whole[0][0][1] + whole[1][1][1] + whole[2][2][1]) / 3.0

        def total(value):
            return jnp.sum(jnp.sum(value, axis=1, keepdims=True), axis=0, keepdims=True)

        sums = jnp.where(lane == 0, total(re), jnp.where(lane == 1, total(im), total(re * re + im * im)))
        mine = (odd * NX + x) * NY + y
        srow[...] = sums
        pl.semaphore_wait(near_sem.at[2], 2 * NX - 1)
        last = z == NZ - 1
        for step in (0, 1):
            dz = jnp.where(last, 1 - step, step)
            end = lax.rem(z + dz, NZ)

            @pl.when(end < EARLY)
            def _():
                for to in (1, 0):
                    for q in SUM_ORDER:
                        for to_x in (0, 1, 3, 2):
                            def send():
                                pltpu.make_async_remote_copy(
                                    src_ref=srow, dst_ref=rows.at[pl.ds(mine, 1)], send_sem=asend_sem, recv_sem=arecv_sem,
                                    device_id=(end * NY + q, to_x * 2 + to), device_id_type=MESH).start()

                            if to == 1:
                                pl.when((dz != 0) | (y != q) | (x != to_x))(send)
                            else:
                                send()

        rows[pl.ds(mine, 1)] = sums
        @pl.when(holder)
        def _():
            for to in range(2):
                for p, value in enumerate((re, im)):
                    phold[to, p:p + 1] = jnp.where(lax.rem(z, NCLASS) < 2, value[to:to + 1], value[2 + to:3 + to])
            other = 1 - 2 * half
            for to, where in ((0, (tm, s - 1)), (0, (tm + other, s - 1)), (1, (tm + other, s))):
                pltpu.make_async_remote_copy(
                    src_ref=phold.at[to], dst_ref=prow, send_sem=asend_sem, recv_sem=precv_sem,
                    device_id=where, device_id_type=MESH).start()
            prow[...] = phold[1]

        @pl.when(jnp.logical_not(holder))
        def _():
            arrived(prow, precv_sem)

        pl.when(z < EARLY)(lambda: arrived(rows.at[pl.ds(0, 2 * NX * NY - 1)], arecv_sem))
        pl.when(z >= EARLY)(lambda: arrived(final, grecv_sem))
        sent(ysend.at[pl.ds(0, NY - 1)], ysend_sem)
        for _, _, by, _, cores in RELAYED:
            @pl.when(y == by)
            def _():
                for _ in cores:
                    sent(yvia.at[0, 0], ysend_sem)

        sent(zrecv.at[:, pl.ds(0, 4 * NZ - 4)], zsend_sem)
        pl.when((z < EARLY - 1) | last)(lambda: sent(rows, asend_sem))
        pl.when(z < EARLY)(lambda: sent(rows.at[pl.ds(0, 2 * NX * NY - 1)], asend_sem))

        @pl.when(holder)
        def _():
            for _ in range(3):
                sent(prow, asend_sem)

    ploop_out[...] = jnp.where(half == 0, prow[:, :64], prow[:, 64:])
    @pl.when(z < EARLY)
    def _():
        grand = jnp.sum(rows[...], axis=0, keepdims=True) / (NY * NCLASS * NSPACE * LANES)
        means = jnp.where(lane < 2, grand * grand, 0.0)
        final[...] = grand - jnp.where(lane == 2, jnp.sum(means, axis=1, keepdims=True), 0.0)

    for start, ends in PASS_ON:
        @pl.when((core == 1) & (z == start))
        def _():
            for end in ends:
                for to in (1, 0):
                    pltpu.make_async_remote_copy(
                        src_ref=final, dst_ref=final, send_sem=asend_sem, recv_sem=grecv_sem,
                        device_id=(end * NY + y, x * 2 + to), device_id_type=MESH).start()
            sent(rows.at[pl.ds(0, 2 * len(ends))], asend_sem)

    stats_out[...] = final[0, :3]


def finish(ploop_in, stats_in, ploop_out, stats_out, sems):
    copies = [pltpu.make_async_copy(ploop_in, ploop_out, sems.at[0]),
              pltpu.make_async_copy(stats_in, stats_out, sems.at[1])]
    for copy in copies:
        copy.start()
    for copy in copies:
        copy.wait()


def on_device(links):
    times_here, sites = links.shape[3:]
    rows = sites // LANES
    view = links.reshape(18, times_here, rows, LANES).transpose(0, 2, 1, 3)
    view = view.reshape(18, 8, 4, times_here, LANES)
    f32 = jnp.float32
    dma = pltpu.SemaphoreType.DMA
    vmem = pl.BlockSpec(memory_space=pltpu.VMEM)
    ploop, stats = pl.pallas_call(
        kernel,
        out_shape=(pltpu.VMEM((2, sites // 64), f32), pltpu.VMEM((3,), f32)),
        in_specs=[pl.BlockSpec(memory_space=pl.ANY)],
        out_specs=(vmem, vmem),
        scratch_shapes=[
            pltpu.VMEM((4, 4, 18, 8, LANES), f32),
            pltpu.VMEM((NY, COORDS, NCLASS, LANES), f32),
            pltpu.VMEM((2, 2, COORDS, NCLASS, LANES), f32),
            pltpu.VMEM((NY, COORDS, 2 * NCLASS, LANES), f32),
            pltpu.VMEM((NY, 18, 2 * NCLASS, LANES), f32),
            pltpu.VMEM((COORDS, 2, 4, LANES), f32),
            pltpu.VMEM((COORDS, 4 * NZ, LANES), f32),
            pltpu.VMEM((2, 2, LANES), f32),
            pltpu.VMEM((2, LANES), f32),
            pltpu.VMEM((1, LANES), f32),
            pltpu.VMEM((2 * NX * NY, LANES), f32),
            pltpu.VMEM((1, LANES), f32),
            pltpu.SemaphoreType.REGULAR((3,)),
            dma((4,)), dma((2,)), dma, dma((NY,)), dma, dma, dma, dma, dma, dma,
        ],
        compiler_params=pltpu.CompilerParams(collective_id=0, has_side_effects=True),
    )(view)
    hbm = pl.BlockSpec(memory_space=pl.ANY)
    return pl.pallas_call(
        finish,
        out_shape=(jax.ShapeDtypeStruct((2, sites // 64), f32), jax.ShapeDtypeStruct((3,), f32)),
        in_specs=[vmem, vmem],
        out_specs=(hbm, hbm),
        scratch_shapes=[dma((2,))],
    )(*(pltpu.with_memory_space_constraint(x, pltpu.VMEM) for x in (ploop, stats)))


def solution(mesh):
    return jax.shard_map(
        on_device, mesh=mesh, in_specs=(P(None, None, None, "tm", "space"),),
        out_specs=(P(None, ("space", "tm")), P()), check_vma=False)
```
